32 devices in a mesh: dp: 2 (over core), seq: 8 (over z, y), head: 2 (over x).
Axes of the slice: x: 2, y: 2, z: 4, core: 2. Of those that a mesh axis runs over, the one named last changes fastest.
Arguments:
- hidden_in: bfloat16 [8, 1024, 1536], P('dp', 'seq'), may hold values from -6 to 6
- segment_ids: int32 [8, 1024], P('dp', 'seq'), may hold values from 0 to 6, as said below
- position_ids: int32 [8, 1024], P('dp', 'seq'), may hold values from 0 to 1017, as said below
- out_cot: bfloat16 [8, 1024, 1536], P('dp', 'seq'), may hold values from -6 to 6
- attn_gain: bfloat16 [1536], replicated, may hold values from 0.5 to 1.5
- w_query: bfloat16 [1536, 1536], P(('dp', 'seq'), 'head'), may hold values from -0.15625 to 0.15625
- b_query: bfloat16 [12, 128], P('head'), may hold values from -3 to 3
- w_key: bfloat16 [1536, 256], P(('dp', 'seq'), 'head'), may hold values from -0.15625 to 0.15625
- b_key: bfloat16 [2, 128], P('head'), may hold values from -3 to 3
- w_value: bfloat16 [1536, 256], P(('dp', 'seq'), 'head'), may hold values from -0.15625 to 0.15625
- b_value: bfloat16 [2, 128], P('head'), may hold values from -3 to 3
- w_out: bfloat16 [1536, 1536], P('head', ('dp', 'seq')), may hold values from -0.625 to 0.625
- ffn_gain: bfloat16 [1536], replicated, may hold values from 0.5 to 1.5
- w_gate: bfloat16 [1536, 8960], P(('dp', 'seq'), 'head'), may hold values from -0.15625 to 0.15625
- w_up: bfloat16 [1536, 8960], P(('dp', 'seq'), 'head'), may hold values from -0.15625 to 0.15625
- w_down: bfloat16 [8960, 1536], P('head', ('dp', 'seq')), may hold values from -0.125 to 0.125
Outputs:
- layer_out: bfloat16 [8, 1024, 1536], P('dp', 'seq')
- input_grad: bfloat16 [8, 1024, 1536], P('dp', 'seq')
- grad_attn_gain: float32 [1536], P(('dp', 'seq'))
- grad_w_query: float32 [1536, 1536], P(('dp', 'seq'), 'head')
- grad_b_query: float32 [12, 128], P('head', ('dp', 'seq'))
- grad_w_key: float32 [1536, 256], P(('dp', 'seq'), 'head')
- grad_b_key: float32 [2, 128], P('head')
- grad_w_value: float32 [1536, 256], P(('dp', 'seq'), 'head')
- grad_b_value: float32 [2, 128], P('head', ('dp', 'seq'))
- grad_w_out: float32 [1536, 1536], P('head', ('dp', 'seq'))
- grad_ffn_gain: float32 [1536], P(('dp', 'seq'))
- grad_w_gate: float32 [1536, 8960], P(('dp', 'seq'), 'head')
- grad_w_up: float32 [1536, 8960], P(('dp', 'seq'), 'head')
- grad_w_down: float32 [8960, 1536], P('head', ('dp', 'seq'))
The draws below stay inside these ranges and needn't reach their ends.
Inputs may be any that keep to these rules, and one draw needn't show every extreme that they name: `segment_ids`: each row's 1024 positions are stored in blocks of 128: block number b holds the row's natural positions b * 64 to b * 64 + 63, then 1024 - (b + 1) * 64 to 1024 - b * 64 - 1, each in rising order. In natural order a row holds 6 documents of uneven lengths with ids 1 to 6, rising, then one or more padding positions with id 0. `position_ids`: in natural order (stored as for segment_ids) the ids count 0, 1, 2 and so on from the start of each document and of the padding.
All inputs are finite; a program needn't handle non-finite values.
Results may differ from the reference program's by a relative error of at most 0.024.
Values may be sent and summed in bfloat16 or wider, within the bound.
A program may use at most 256 MiB of HBM per device.

```python
import math
import jax
import jax.numpy as jnp
from jax import lax

D = 1536
HQ = 12
KVH = 2
HD = 128
FF = 8960
SPAN = 64
NDOC = 6
LENGTH = 1024
ROWS = 8


def natural_row(row_key, longest):
    pad_key, cut_key = jax.random.split(row_key)
    padding = jax.random.randint(pad_key, (), 1, LENGTH // 8 + 1).astype(jnp.int32)
    padding = jnp.where(longest, 1, padding).astype(jnp.int32)
    filled = LENGTH - padding
    shuffled = jax.random.permutation(cut_key, LENGTH - 1).astype(jnp.int32) + 1
    beyond = (shuffled >= filled).astype(jnp.int32)
    ranked = shuffled[jnp.argsort(beyond, stable=True)]
    tail_cuts = filled - (NDOC - 1) + jnp.arange(NDOC - 1, dtype=jnp.int32)
    cut_points = jnp.where(longest, tail_cuts, ranked[:NDOC - 1]).astype(jnp.int32)
    places = jnp.arange(LENGTH, dtype=jnp.int32)
    starts = jnp.concatenate([jnp.zeros((1,), jnp.int32), cut_points, jnp.reshape(filled, (1,))])
    passed = places[:, None] >= starts[None, :]
    doc_number = jnp.sum(passed.astype(jnp.int32), axis=1)
    segment = jnp.where(places >= filled, 0, doc_number)
    doc_start = jnp.max(jnp.where(passed, starts[None, :], 0), axis=1)
    return (segment, places - doc_start)


def reorder_row(row_values):
    halves = LENGTH // (2 * SPAN)
    blocks_all = row_values.reshape(2 * halves, SPAN)
    leading = blocks_all[:halves]
    trailing = blocks_all[halves:][::-1]
    return jnp.stack([leading, trailing], axis=1).reshape(LENGTH)


def labels(key):
    row_keys = jax.random.split(jax.random.fold_in(key, 11), ROWS)
    longest = jnp.arange(ROWS, dtype=jnp.int32) == 0
    segment, position = jax.vmap(natural_row)(row_keys, longest)
    return (jax.vmap(reorder_row)(segment), jax.vmap(reorder_row)(position))


def draw_segment_ids(key, part):
    return labels(key)[0]


def draw_position_ids(key, part):
    return labels(key)[1]


def spiked(values, own_key, source, target, blocks, factor):
    def block_of(dim):
        return (jnp.arange(values.shape[dim]) // (values.shape[dim] // blocks)).reshape((-1,) + (1,) * (values.ndim - 1 - dim))

    near = jax.random.permutation(own_key, blocks)[block_of(target)]
    second = (block_of(target) + blocks // 2) % blocks
    return jnp.where((block_of(source) == near) | (block_of(source) == second), factor * values, values)


def block_scale(key, shape, pieces, smallest, high):
    factor_of = 1.0
    for dim, blocks in pieces:
        steps = jax.random.uniform(jax.random.fold_in(jax.random.fold_in(key, 6), dim), (blocks,), jnp.float32, smallest / len(pieces), high / len(pieces))
        factor_of = factor_of * jnp.repeat(jnp.exp(steps), shape[dim] // blocks).reshape((-1,) + (1,) * (len(shape) - 1 - dim))
    return factor_of


def gaussian(own_key, extent, deviation, bound, cuts=(), held_as=jnp.bfloat16):
    loudness = block_scale(own_key, extent, cuts, -0.22, 0.18) if cuts else 1.0
    values = jax.random.normal(own_key, extent, jnp.float32) * deviation * loudness
    return jnp.minimum(jnp.maximum(values, -bound), bound).astype(held_as)


def bell_draw_with(stream_key, dims, deviation, bound, shards, heavy, held_as=jnp.bfloat16):
    array = deviation * jax.random.normal(stream_key, dims, jnp.float32)
    if shards:
        array = array * block_scale(stream_key, dims, shards, -0.22, 0.18)
    return jnp.clip(spiked(array, jax.random.fold_in(stream_key, 3), *heavy), -bound, bound).astype(held_as)


def setup_inputs(seed: int = 0) -> dict:
    streams_of = jax.random.split(jax.random.key(seed), 17)
    hidden_in = bell_draw_with(streams_of[0], (ROWS, LENGTH, D), 1.0, 6.0, ((0, 2), (1, 8)), (1, 2, 8, 2.0))
    segment_ids = draw_segment_ids(jax.random.fold_in(streams_of[16], 71), 0)
    position_ids = draw_position_ids(jax.random.fold_in(streams_of[16], 71), 0)
    out_cot = bell_draw_with(streams_of[3], (ROWS, LENGTH, D), 1.0, 6.0, ((0, 2), (1, 8)), (1, 2, 8, 2.0))
    attn_gain = jnp.clip(1.0 + 0.1 * jax.random.normal(streams_of[4], (D,), jnp.float32), 0.5, 1.5).astype(jnp.bfloat16)
    w_query = gaussian(streams_of[5], (D, HQ * HD), D ** -0.5, 0.15625, ((0, 16), (1, 2)))
    b_query = gaussian(streams_of[6], (HQ, HD), 0.5, 3.0, ((0, 2),))
    w_key = gaussian(streams_of[7], (D, KVH * HD), D ** -0.5, 0.15625, ((0, 16), (1, 2)))
    b_key = gaussian(streams_of[8], (KVH, HD), 0.5, 3.0, ((0, 2),))
    w_value = gaussian(streams_of[9], (D, KVH * HD), D ** -0.5, 0.15625, ((0, 16), (1, 2)))
    b_value = gaussian(streams_of[10], (KVH, HD), 0.5, 3.0, ((0, 2),))
    w_out = gaussian(streams_of[11], (HQ * HD, D), (HQ * HD // 16) ** -0.5, 0.625, ((0, 2), (1, 16)))
    ffn_gain = jnp.clip(1.0 + 0.1 * jax.random.normal(streams_of[12], (D,), jnp.float32), 0.5, 1.5).astype(jnp.bfloat16)
    w_gate = gaussian(streams_of[13], (D, FF), D ** -0.5, 0.15625, ((0, 16), (1, 2)))
    w_up = gaussian(streams_of[14], (D, FF), D ** -0.5, 0.15625, ((0, 16), (1, 2)))
    w_down = gaussian(streams_of[15], (FF, D), (FF // 4) ** -0.5, 0.125, ((0, 2), (1, 16)))
    return dict(hidden_in=hidden_in, segment_ids=segment_ids, position_ids=position_ids, out_cot=out_cot, attn_gain=attn_gain, w_query=w_query, b_query=b_query, w_key=w_key, b_key=b_key, w_value=w_value, b_value=b_value, w_out=w_out, ffn_gain=ffn_gain, w_gate=w_gate, w_up=w_up, w_down=w_down)


EPSILON = 1e-06
THETA = 1000000.0
HIGH = lax.Precision.HIGHEST

@jax.custom_vjp
def low(v):
    return lax.optimization_barrier(v.astype(jnp.bfloat16)).astype(jnp.float32)

@jax.custom_vjp
def low_back(v):
    return v

def low_keep(v):
    return (low(v), None)

def low_pass(kept, grad):
    return (grad,)

def back_keep(v):
    return (v, None)

def back_low(kept, grad):
    return (low(grad),)
low.defvjp(low_keep, low_pass)
low_back.defvjp(back_keep, back_low)

def matmul(left, right):
    return jnp.dot(left, right, precision=HIGH, preferred_element_type=jnp.float32)

def normalize(values, gain):
    return values * lax.rsqrt(lax.optimization_barrier(jnp.mean(values * values, axis=-1, keepdims=True)) + EPSILON) * gain

def rotary(values, position):
    half_size = values.shape[-1] // 2
    frequency = THETA ** (-jnp.arange(half_size, dtype=jnp.float32) * 2.0 / values.shape[-1])
    angles = position.astype(jnp.float32)[:, None] * frequency[None, :]
    cosine = jnp.cos(angles)[:, None, :]
    sine_table = jnp.sin(angles)[:, None, :]
    first_half = values[..., :half_size]
    second_half = values[..., half_size:]
    return jnp.concatenate([first_half * cosine - second_half * sine_table, second_half * cosine + first_half * sine_table], axis=-1)

def attend(queries, key_rot, values, segment, position):
    length = queries.shape[0]
    block_rows = math.gcd(length, 512)
    block_count = length // block_rows
    factor = HD ** (-0.5)

    def one_block(inputs):
        query_block, seg_block, pos_block = inputs
        scores = low_back(jnp.einsum('qkgd,tkd->kgqt', query_block, key_rot, precision=HIGH) * factor)
        allowed = (seg_block[:, None] == segment[None, :]) & (position[None, :] <= pos_block[:, None])
        scores = jnp.where(allowed[None, None], scores, -1e+30)
        top_score = lax.optimization_barrier(jnp.max(scores, axis=-1, keepdims=True))
        exp_terms = jnp.exp(scores - top_score)
        probs = exp_terms / lax.optimization_barrier(jnp.sum(exp_terms, axis=-1, keepdims=True))
        weights = low(probs)
        return jnp.einsum('kgqt,tkd->qkgd', weights, values, precision=HIGH)
    blocks = lax.map(jax.checkpoint(one_block), (queries.reshape(block_count, block_rows, KVH, HQ // KVH, HD), segment.reshape(block_count, block_rows), position.reshape(block_count, block_rows)))
    return blocks.reshape(length, HQ * HD)

def layer(hidden, params, segment, position):
    attn_gain, w_query, b_query, w_key, b_key, w_value, b_value, w_out, ffn_gain, w_gate, w_up, w_down = params
    length = hidden.shape[0]
    normed = low(normalize(hidden, attn_gain))
    query_pre = low_back(matmul(normed, w_query) + b_query.reshape(-1)).reshape(length, HQ, HD)
    key_pre = low_back(matmul(normed, w_key) + b_key.reshape(-1)).reshape(length, KVH, HD)
    values = low(low_back(matmul(normed, w_value) + b_value.reshape(-1))).reshape(length, KVH, HD)
    queries = low(rotary(query_pre, position)).reshape(length, KVH, HQ // KVH, HD)
    key_rot = low(rotary(key_pre, position))
    mixed = low(low_back(attend(queries, key_rot, values, segment, position)))
    middle = hidden + low_back(matmul(mixed, w_out))
    normed_two = low(normalize(middle, ffn_gain))
    gate_pre = low_back(matmul(normed_two, w_gate))
    up_pre = low_back(matmul(normed_two, w_up))
    product = low(low_back(jax.nn.silu(gate_pre) * up_pre))
    return middle + low_back(matmul(product, w_down))

def reference(hidden_in, segment_ids, position_ids, out_cot, attn_gain, w_query, b_query, w_key, b_key, w_value, b_value, w_out, ffn_gain, w_gate, w_up, w_down):
    params = tuple((item.astype(jnp.float32) for item in (attn_gain, w_query, b_query, w_key, b_key, w_value, b_value, w_out, ffn_gain, w_gate, w_up, w_down)))

    def row_step(totals, row_inputs):
        hidden_row, seg_row, pos_row, cot_row = row_inputs
        hidden_row = hidden_row.astype(jnp.float32)
        result, pullback = jax.vjp(lambda hid, weights: layer(hid, weights, seg_row, pos_row), hidden_row, params)
        live_rows = (seg_row != 0).astype(jnp.float32)[:, None]
        grad_hidden, grad_params = pullback(cot_row.astype(jnp.float32) * live_rows)
        totals = jax.tree.map(lambda first, second: first + second, totals, grad_params)
        return (totals, (result.astype(jnp.bfloat16), grad_hidden.astype(jnp.bfloat16)))
    zero_grads = jax.tree.map(jnp.zeros_like, params)
    totals, (outputs, input_grads) = lax.scan(row_step, zero_grads, (hidden_in, segment_ids, position_ids, out_cot))
    g_attn_gain, g_query, g_bquery, g_key, g_bkey, g_value, g_bvalue, g_out, g_ffn_gain, g_gate, g_up, g_down = totals
    return (outputs, input_grads, g_attn_gain, g_query, g_bquery, g_key, g_bkey, g_value, g_bvalue, g_out, g_ffn_gain, g_gate, g_up, g_down)
```

```python
import functools

import jax
import jax.numpy as jnp
from jax import lax
from jax.experimental import pallas as pl
from jax.experimental.pallas import tpu as pltpu
from jax.sharding import PartitionSpec as P

EPSILON = 1e-06
THETA = 1000000.0
MASKED = -1e30
LANES = 128
BF16 = jnp.bfloat16
F32 = jnp.float32


def rope_tables(position, head_size):
    half_size = head_size // 2
    frequency = THETA ** (-jnp.arange(half_size, dtype=F32) * 2.0 / head_size)
    angles = position.astype(F32)[:, None] * frequency[None, :]
    return jnp.cos(angles), jnp.sin(angles)


def rotate(values, cosine, sine_table, direction):
    half_size = values.shape[-1] // 2
    first_half = values[..., :half_size]
    second_half = values[..., half_size:]
    return jnp.concatenate(
        [
            first_half * cosine - direction * (second_half * sine_table),
            second_half * cosine + direction * (first_half * sine_table),
        ],
        axis=-1,
    )


def plain_dot(left, right):
    return jnp.dot(left, right, preferred_element_type=F32)


def grad_of_weight(left, right):
    return lax.dot_general(left, right, (((0,), (0,)), ((), ())), preferred_element_type=F32)


def through_weight(left, right):
    return lax.dot_general(left, right, (((1,), (1,)), ((), ())), preferred_element_type=F32)


def norm_scale(values):
    return lax.rsqrt(jnp.mean(values * values, axis=-1, keepdims=True) + EPSILON)


def norm_back(grad_in, values, scale_rows, gain):
    scaled = grad_in * gain
    cubed = scale_rows * scale_rows * scale_rows
    return scale_rows * scaled - values * cubed * jnp.mean(scaled * values, axis=-1, keepdims=True)


def flip(values, axis, mask):
    size = lax.axis_size(axis)
    return lax.ppermute(values, axis, [(i, i ^ mask) for i in range(size)])


def flip_pair(values, core_mask, seq_mask):
    if not core_mask:
        return flip(values, "seq", seq_mask)
    if not seq_mask:
        return flip(values, "dp", core_mask)
    cores, places = lax.axis_size("dp"), lax.axis_size("seq")
    pairs = [
        (c * places + s, (c ^ core_mask) * places + (s ^ seq_mask))
        for c in range(cores)
        for s in range(places)
    ]
    return lax.ppermute(values, ("dp", "seq"), pairs)


def after(values, gate):
    return lax.optimization_barrier((values, gate))[0]


def put(buffer, piece, *index):
    for _ in index:
        piece = piece[None]
    start = tuple(index) + (0,) * (buffer.ndim - len(index))
    return lax.dynamic_update_slice(buffer, piece, start)


def take(buffer, index, axis=0):
    return lax.dynamic_index_in_dim(buffer, index, axis, keepdims=False)


def allowed_keys(seg_q, pos_q, seg_k, pos_k):
    return (seg_q == seg_k) & (pos_k <= pos_q)


def dot_nt(left, right):
    return lax.dot_general(left, right, (((1,), (1,)), ((), ())), preferred_element_type=F32)


def dot_tn(left, right):
    return lax.dot_general(left, right, (((0,), (0,)), ((), ())), preferred_element_type=F32)


def probabilities(query, keys, allowed, factor):
    scores = jnp.where(allowed, dot_nt(query, keys) * factor, MASKED)
    top = jnp.max(scores, axis=-1, keepdims=True)
    terms = jnp.where(allowed, jnp.exp(scores - top), 0.0)
    return terms / jnp.sum(terms, axis=-1, keepdims=True)


def attend_kernel(heads, head_size, factor, q_ref, kv_ref, sq_ref, pq_ref, sk_ref, pk_ref, o_ref):
    allowed = allowed_keys(sq_ref[0], pq_ref[0], sk_ref[0], pk_ref[0])
    keys = kv_ref[0, :, :head_size]
    values = kv_ref[0, :, head_size:]
    for head in range(heads):
        lanes = slice(head * head_size, (head + 1) * head_size)
        probs = probabilities(q_ref[0, :, lanes], keys, allowed, factor)
        o_ref[0, :, lanes] = jnp.dot(
            probs.astype(BF16), values, preferred_element_type=F32
        ).astype(BF16)


def attend_back_kernel(
    heads, head_size, factor, q_ref, do_ref, kv_ref, sq_ref, pq_ref, sk_ref, pk_ref, dq_ref, dkv_ref, acc
):
    allowed = allowed_keys(sq_ref[0], pq_ref[0], sk_ref[0], pk_ref[0])
    keys = kv_ref[0, :, :head_size]
    values = kv_ref[0, :, head_size:]
    for head in range(heads):
        lanes = slice(head * head_size, (head + 1) * head_size)
        query = q_ref[0, :, lanes]
        d_out = do_ref[0, :, lanes]
        probs = probabilities(query, keys, allowed, factor)
        d_probs = dot_nt(d_out, values)
        delta = jnp.sum(probs * d_probs, axis=-1, keepdims=True)
        d_scores = (probs * (d_probs - delta)).astype(BF16)
        dq_ref[0, :, lanes] = jnp.dot(d_scores, keys, preferred_element_type=F32) * factor
        d_key = dot_tn(d_scores, query) * factor
        d_value = dot_tn(probs.astype(BF16), d_out)
        if head == 0:
            acc[:, :head_size] = d_key
            acc[:, head_size:] = d_value
        else:
            acc[:, :head_size] += d_key
            acc[:, head_size:] += d_value
    dkv_ref[0] = acc[...].astype(BF16)


def row_spec(*shape):
    return pl.BlockSpec((1,) + shape, lambda row: (row,) + (0,) * len(shape))


def attend(queries, all_kv, marks, heads, head_size, factor):
    rows, width, wide = queries.shape
    length = all_kv.shape[1]
    return pl.pallas_call(
        functools.partial(attend_kernel, heads, head_size, factor),
        grid=(rows,),
        out_shape=jax.ShapeDtypeStruct((rows, width, wide), BF16),
        in_specs=[
            row_spec(width, wide),
            row_spec(length, 2 * head_size),
            row_spec(width, 1),
            row_spec(width, 1),
            row_spec(1, length),
            row_spec(1, length),
        ],
        out_specs=row_spec(width, wide),
        cost_estimate=pl.CostEstimate(
            flops=4 * rows * width * wide * length,
            bytes_accessed=4 * rows * (width * wide + length * head_size),
            transcendentals=rows * width * heads * length,
        ),
        name="attend",
    )(queries, all_kv, *marks)


def attend_back(queries, d_mixed, all_kv, marks, heads, head_size, factor):
    rows, width, wide = queries.shape
    length = all_kv.shape[1]
    return pl.pallas_call(
        functools.partial(attend_back_kernel, heads, head_size, factor),
        grid=(rows,),
        out_shape=(
            jax.ShapeDtypeStruct((rows, width, wide), F32),
            jax.ShapeDtypeStruct((rows, length, 2 * head_size), BF16),
        ),
        in_specs=[
            row_spec(width, wide),
            row_spec(width, wide),
            row_spec(length, 2 * head_size),
            row_spec(width, 1),
            row_spec(width, 1),
            row_spec(1, length),
            row_spec(1, length),
        ],
        out_specs=(row_spec(width, wide), row_spec(length, 2 * head_size)),
        scratch_shapes=[pltpu.VMEM((length, 2 * head_size), F32)],
        cost_estimate=pl.CostEstimate(
            flops=10 * rows * width * wide * length,
            bytes_accessed=8 * rows * (width * wide + length * head_size),
            transcendentals=rows * width * heads * length,
        ),
        name="attend_back",
    )(queries, d_mixed, all_kv, *marks)


def gather_rows(piece, core, place):
    places = lax.axis_size("seq")
    own = jnp.zeros((places,) + piece.shape, piece.dtype)
    for k in range(places):
        part = flip(piece, "seq", k) if k else piece
        own = put(own, part, place ^ k)
    other = flip(own, "dp", 1)
    both = jnp.zeros((2,) + own.shape, piece.dtype)
    both = put(put(both, own, core), other, 1 - core)
    return both.reshape(-1, piece.shape[-1])


def scatter_rows(grad, core, place):
    places = lax.axis_size("seq")
    blocks = grad.astype(BF16).reshape(2, places, -1, grad.shape[-1])
    other = flip(take(blocks, 1 - core), "dp", 1)
    mine = take(blocks, core).astype(F32) + other.astype(F32)
    mine_low = mine.astype(BF16)
    total = take(mine, place)
    for k in range(1, places):
        total = total + flip(take(mine_low, place ^ k), "seq", k).astype(F32)
    return total


def total_over(values, axes):
    for axis in axes:
        bit = 1
        while bit < lax.axis_size(axis):
            values = values + flip(values, axis, bit)
            bit *= 2
    return values


def sum_heads(part):
    low = lax.reduce_precision(part, 8, 7).astype(BF16)
    return low.astype(F32) + flip(low, "head", 1).astype(F32)


def spread_tokens(values):
    far = flip(values, "seq", 1)
    return jnp.concatenate([values, flip(values, "dp", 1), far, flip(far, "dp", 1)], axis=0)


def collect_tokens(part):
    blocks = part.reshape((2, 2, -1) + part.shape[1:])
    low = blocks.astype(BF16)
    other = flip(low[:, 1], "dp", 1).astype(F32)
    near = blocks[0, 0] + other[0]
    far = (blocks[1, 0] + other[1]).astype(BF16)
    return near + flip(far, "seq", 1).astype(F32)


def on_device(
    hidden_in,
    segment_ids,
    position_ids,
    out_cot,
    attn_gain,
    w_query,
    b_query,
    w_key,
    b_key,
    w_value,
    b_value,
    w_out,
    ffn_gain,
    w_gate,
    w_up,
    w_down,
):
    row_count, row_width, model_width = hidden_in.shape
    tokens = row_count * row_width
    heads, head_size = b_query.shape
    wide = heads * head_size
    factor = head_size ** (-0.5)
    places = lax.axis_size("seq")
    planes = places // 2
    core = lax.axis_index("dp")
    place = lax.axis_index("seq")
    plane = place // 2
    side = place % 2
    shard = w_gate.shape[0]
    units = w_gate.shape[1]
    block = -(-units // (4 * LANES)) * LANES

    marks_own = jnp.stack([segment_ids, position_ids])
    marks_all = jnp.concatenate(
        [flip(marks_own, "seq", k) if k else marks_own for k in range(places)], axis=2
    )
    marks = (
        segment_ids[:, :, None],
        position_ids[:, :, None],
        marks_all[0][:, None, :],
        marks_all[1][:, None, :],
    )

    full_qkv = gather_rows(jnp.concatenate([w_query, w_key, w_value], axis=1), core, place)

    hidden = hidden_in.reshape(tokens, model_width).astype(F32)
    scale_one = norm_scale(hidden)
    gain_one = attn_gain.astype(F32)
    normed = (hidden * scale_one * gain_one).astype(BF16)
    cosine, sine_table = rope_tables(position_ids.reshape(tokens), head_size)
    bias = jnp.concatenate([b_query.reshape(-1), b_key.reshape(-1), b_value.reshape(-1)])
    qkv = plain_dot(normed, full_qkv) + bias.astype(F32)
    queries = rotate(
        qkv[:, :wide].reshape(tokens, heads, head_size),
        cosine[:, None, :],
        sine_table[:, None, :],
        1.0,
    ).astype(BF16)
    queries = queries.reshape(row_count, row_width, wide)
    key_rot = rotate(qkv[:, wide : wide + head_size], cosine, sine_table, 1.0).astype(BF16)
    local_kv = jnp.concatenate([key_rot, qkv[:, wide + head_size :].astype(BF16)], axis=-1)
    local_kv = local_kv.reshape(row_count, row_width, 2 * head_size)
    all_kv = jnp.concatenate(
        [flip(local_kv, "seq", k) if k else local_kv for k in range(places)], axis=1
    )

    full_out = gather_rows(after(w_out.T, full_qkv), core, place)

    stacked = jnp.stack([w_gate, w_up, w_down.T])
    stacked = jnp.pad(stacked, ((0, 0), (0, 0), (0, 4 * block - units)))
    stacked = stacked.reshape(3, shard, 4, block).transpose(2, 0, 1, 3)
    stacked = after(stacked, full_qkv)
    here = core * 2 + side
    plane_weights = jnp.zeros((3, 2, 2, shard, block), BF16)
    for m in range(4):
        piece = take(stacked, here ^ m)
        if m:
            piece = flip_pair(piece, m // 2, m % 2)
        start = (0, core ^ (m // 2), side ^ (m % 2), 0, 0)
        plane_weights = lax.dynamic_update_slice(
            plane_weights, piece[:, None, None], start
        )
    full_ffn = []
    for i in range(3):
        whole = jnp.zeros((2, planes, 2, shard, block), BF16)
        for k in range(planes):
            piece = plane_weights[i]
            if k:
                piece = flip(piece, "seq", 2 * k)
            whole = lax.dynamic_update_slice(whole, piece[:, None], (0, plane ^ k, 0, 0, 0))
        full_ffn.append(whole.reshape(model_width, block))
    full_gate, full_up, full_down = full_ffn

    live_rows = (segment_ids != 0).astype(F32).reshape(tokens, 1)
    cotangent = out_cot.reshape(tokens, model_width).astype(F32) * live_rows
    cot_low = spread_tokens(after(cotangent.astype(BF16), full_qkv))

    mixed = attend(queries, all_kv, marks, heads, head_size, factor).reshape(tokens, wide)
    middle = hidden + sum_heads(through_weight(mixed, full_out))
    scale_two = norm_scale(middle)
    gain_two = ffn_gain.astype(F32)
    normed_two = spread_tokens((middle * scale_two * gain_two).astype(BF16))

    gate_pre = plain_dot(normed_two, full_gate)
    up_pre = plain_dot(normed_two, full_up)
    sigmoid_gate = jax.nn.sigmoid(gate_pre)
    activated = gate_pre * sigmoid_gate
    product = (activated * up_pre).astype(BF16)
    grad_down = grad_of_weight(cot_low, product)
    d_product = plain_dot(cot_low, full_down).astype(BF16).astype(F32)
    d_gate = (d_product * up_pre * sigmoid_gate * (1.0 + gate_pre * (1.0 - sigmoid_gate))).astype(
        BF16
    )
    d_up = (d_product * activated).astype(BF16)
    back_two = through_weight(d_gate, full_gate) + through_weight(d_up, full_up)
    back_two = sum_heads(collect_tokens(back_two))
    grad_gate = grad_of_weight(normed_two, d_gate)
    grad_up = grad_of_weight(normed_two, d_up)
    result = middle + sum_heads(collect_tokens(through_weight(product, full_down)))
    layer_out = result.astype(BF16).reshape(row_count, row_width, model_width)

    ffn_sums = []
    for grad in (grad_down, grad_gate, grad_up):
        blocks = grad.astype(BF16).reshape(2, planes, 2, shard, block)
        total = take(blocks, plane, 1).astype(F32)
        for k in range(1, planes):
            total = total + flip(take(blocks, plane ^ k, 1), "seq", 2 * k).astype(F32)
        total = total.astype(BF16).reshape(4, shard, block)
        whole = jnp.zeros((4, shard, block), F32)
        for m in range(4):
            piece = take(total, here ^ m)
            if m:
                piece = flip_pair(piece, m // 2, m % 2)
            whole = put(whole, piece.astype(F32), here ^ m)
        ffn_sums.append(whole.transpose(1, 0, 2).reshape(shard, 4 * block)[:, :units])
    down_sum, gate_sum, up_sum = ffn_sums
    down_sum = down_sum.T

    gain_two_grad = jnp.sum(back_two * middle * scale_two, axis=0)
    d_middle = cotangent + norm_back(back_two, middle, scale_two, gain_two)
    d_middle_low = d_middle.astype(BF16)
    out_sum = scatter_rows(grad_of_weight(d_middle_low, mixed), core, place).T
    d_mixed = plain_dot(d_middle_low, full_out).astype(BF16)

    d_query, d_kv_all = attend_back(
        queries,
        d_mixed.reshape(row_count, row_width, wide),
        all_kv,
        marks,
        heads,
        head_size,
        factor,
    )
    d_kv = d_kv_all[:, :row_width].astype(F32)
    for k in range(1, places):
        piece = d_kv_all[:, k * row_width : (k + 1) * row_width]
        d_kv = d_kv + flip(piece, "seq", k).astype(F32)
    d_kv = d_kv.reshape(tokens, 2 * head_size)
    d_key = rotate(d_kv[:, :head_size], cosine, sine_table, -1.0).astype(BF16)
    d_value = d_kv[:, head_size:].astype(BF16)
    d_query = rotate(
        d_query.reshape(tokens, heads, head_size),
        cosine[:, None, :],
        sine_table[:, None, :],
        -1.0,
    ).astype(BF16)
    d_qkv = jnp.concatenate([d_query.reshape(tokens, wide), d_key, d_value], axis=-1)
    qkv_sum = scatter_rows(grad_of_weight(normed, d_qkv), core, place)
    back_part = through_weight(d_qkv, full_qkv)
    back_one = sum_heads(back_part)
    d_hidden = d_middle + norm_back(back_one, hidden, scale_one, gain_one)
    input_grad = d_hidden.astype(BF16).reshape(row_count, row_width, model_width)

    bias_grad = jnp.sum(d_qkv.astype(F32), axis=0)
    gain_one_grad = jnp.sum(back_one * hidden * scale_one, axis=0)
    vectors = total_over(jnp.concatenate([bias_grad, gain_two_grad, gain_one_grad]), ("dp", "seq"))
    index = core * places + place
    replicas = 2 * places
    narrow = head_size // replicas
    bias_sums = vectors[: wide + 2 * head_size].reshape(heads + 2, head_size)
    bias_mine = lax.dynamic_slice_in_dim(bias_sums, index * narrow, narrow, 1)
    gains = vectors[wide + 2 * head_size :].reshape(2, replicas, model_width // replicas)
    gains_mine = take(gains, index, 1)
    return (
        layer_out,
        input_grad,
        gains_mine[1],
        qkv_sum[:, :wide],
        bias_mine[:heads],
        qkv_sum[:, wide : wide + head_size],
        bias_sums[heads : heads + 1],
        qkv_sum[:, wide + head_size :],
        bias_mine[heads + 1 :],
        out_sum,
        gains_mine[0],
        gate_sum,
        up_sum,
        down_sum,
    )


def solution(mesh):
    placed = (
        P("dp", "seq", None),
        P("dp", "seq"),
        P("dp", "seq"),
        P("dp", "seq", None),
        P(),
        P(("dp", "seq"), "head"),
        P("head", None),
        P(("dp", "seq"), "head"),
        P("head", None),
        P(("dp", "seq"), "head"),
        P("head", None),
        P("head", ("dp", "seq")),
        P(),
        P(("dp", "seq"), "head"),
        P(("dp", "seq"), "head"),
        P("head", ("dp", "seq")),
    )
    return jax.shard_map(
        on_device,
        mesh=mesh,
        in_specs=placed,
        out_specs=(
            P("dp", "seq", None),
            P("dp", "seq", None),
            P(("dp", "seq")),
            P(("dp", "seq"), "head"),
            P("head", ("dp", "seq")),
            P(("dp", "seq"), "head"),
            P("head", None),
            P(("dp", "seq"), "head"),
            P("head", ("dp", "seq")),
            P("head", ("dp", "seq")),
            P(("dp", "seq")),
            P(("dp", "seq"), "head"),
            P(("dp", "seq"), "head"),
            P("head", ("dp", "seq")),
        ),
        check_vma=False,
    )
```

```python
import functools

import jax
import jax.numpy as jnp
from jax import lax
from jax.experimental import pallas as pl
from jax.experimental.pallas import tpu as pltpu
from jax.sharding import PartitionSpec as P

EPSILON = 1e-06
THETA = 1000000.0
MASKED = -1e30
LANES = 128
BF16 = jnp.bfloat16
F32 = jnp.float32
MESH = pl.DeviceIdType.MESH


def rope_tables(position, head_size):
    half_size = head_size // 2
    frequency = THETA ** (-jnp.arange(half_size, dtype=F32) * 2.0 / head_size)
    angles = position.astype(F32)[:, None] * frequency[None, :]
    return jnp.cos(angles), jnp.sin(angles)


def rotate(values, cosine, sine_table, direction):
    half_size = values.shape[-1] // 2
    first_half = values[..., :half_size]
    second_half = values[..., half_size:]
    return jnp.concatenate(
        [
            first_half * cosine - direction * (second_half * sine_table),
            second_half * cosine + direction * (first_half * sine_table),
        ],
        axis=-1,
    )


def xor(index, mask):
    out = index
    bit = 1
    while bit <= mask:
        if mask & bit:
            out = out + bit - 2 * bit * lax.rem(lax.div(index, bit), 2)
        bit *= 2
    return out


def plain_dot(left, right):
    return jnp.dot(left, right, preferred_element_type=F32)


def grad_of_weight(left, right):
    return lax.dot_general(left, right, (((0,), (0,)), ((), ())), preferred_element_type=F32)


def through_weight(left, right):
    return lax.dot_general(left, right, (((1,), (1,)), ((), ())), preferred_element_type=F32)


def norm_scale(values):
    return lax.rsqrt(jnp.mean(values * values, axis=-1, keepdims=True) + EPSILON)


def norm_back(grad_in, values, scale_rows, gain):
    scaled = grad_in * gain
    cubed = scale_rows * scale_rows * scale_rows
    return scale_rows * scaled - values * cubed * jnp.mean(scaled * values, axis=-1, keepdims=True)


def flip(values, axis, mask):
    size = lax.axis_size(axis)
    return lax.ppermute(values, axis, [(i, i ^ mask) for i in range(size)])


def flip_pair(values, core_mask, seq_mask):
    if not core_mask:
        return flip(values, "seq", seq_mask)
    if not seq_mask:
        return flip(values, "dp", core_mask)
    cores, places = lax.axis_size("dp"), lax.axis_size("seq")
    pairs = [
        (c * places + s, (c ^ core_mask) * places + (s ^ seq_mask))
        for c in range(cores)
        for s in range(places)
    ]
    return lax.ppermute(values, ("dp", "seq"), pairs)


def after(values, gate):
    return lax.optimization_barrier((values, gate))[0]


def put(buffer, piece, *index):
    for _ in index:
        piece = piece[None]
    start = tuple(index) + (0,) * (buffer.ndim - len(index))
    return lax.dynamic_update_slice(buffer, piece, start)


def take(buffer, index, axis=0):
    return lax.dynamic_index_in_dim(buffer, index, axis, keepdims=False)


def allowed_keys(seg_q, pos_q, seg_k, pos_k):
    return (seg_q == seg_k) & (pos_k <= pos_q)


def dot_nt(left, right):
    return lax.dot_general(left, right, (((1,), (1,)), ((), ())), preferred_element_type=F32)


def dot_tn(left, right):
    return lax.dot_general(left, right, (((0,), (0,)), ((), ())), preferred_element_type=F32)


def probabilities(query, keys, allowed, factor):
    scores = jnp.where(allowed, dot_nt(query, keys) * factor, MASKED)
    top = jnp.max(scores, axis=-1, keepdims=True)
    terms = jnp.where(allowed, jnp.exp(scores - top), 0.0)
    return terms / jnp.sum(terms, axis=-1, keepdims=True)


def attend_kernel(heads, head_size, factor, q_ref, kv_ref, sq_ref, pq_ref, sk_ref, pk_ref, o_ref):
    allowed = allowed_keys(sq_ref[0], pq_ref[0], sk_ref[0], pk_ref[0])
    joint = kv_ref[:, 0].reshape(-1, 2 * head_size)
    keys = joint[:, :head_size]
    values = joint[:, head_size:]
    for head in range(heads):
        lanes = slice(head * head_size, (head + 1) * head_size)
        probs = probabilities(q_ref[0, :, lanes], keys, allowed, factor)
        o_ref[0, :, lanes] = jnp.dot(
            probs.astype(BF16), values, preferred_element_type=F32
        ).astype(BF16)


def attend_back_kernel(
    heads, head_size, factor, q_ref, do_ref, kv_ref, sq_ref, pq_ref, sk_ref, pk_ref, dq_ref, dkv_ref, acc
):
    allowed = allowed_keys(sq_ref[0], pq_ref[0], sk_ref[0], pk_ref[0])
    joint = kv_ref[:, 0].reshape(-1, 2 * head_size)
    keys = joint[:, :head_size]
    values = joint[:, head_size:]
    for head in range(heads):
        lanes = slice(head * head_size, (head + 1) * head_size)
        query = q_ref[0, :, lanes]
        d_out = do_ref[0, :, lanes]
        probs = probabilities(query, keys, allowed, factor)
        d_probs = dot_nt(d_out, values)
        delta = jnp.sum(probs * d_probs, axis=-1, keepdims=True)
        d_scores = (probs * (d_probs - delta)).astype(BF16)
        dq_ref[0, :, lanes] = jnp.dot(d_scores, keys, preferred_element_type=F32) * factor
        d_key = dot_tn(d_scores, query) * factor
        d_value = dot_tn(probs.astype(BF16), d_out)
        if head == 0:
            acc[:, :head_size] = d_key
            acc[:, head_size:] = d_value
        else:
            acc[:, :head_size] += d_key
            acc[:, head_size:] += d_value
    dkv_ref[:, 0] = acc[...].astype(BF16).reshape(dkv_ref.shape[0], -1, 2 * head_size)


def row_spec(*shape):
    return pl.BlockSpec((1,) + shape, lambda row: (row,) + (0,) * len(shape))


def keys_spec(places, *shape):
    return pl.BlockSpec(
        (places, 1) + shape, lambda row: (0, row) + (0,) * len(shape)
    )


def attend(queries, all_kv, marks, heads, head_size, factor):
    rows, width, wide = queries.shape
    places = all_kv.shape[0]
    length = places * width
    return pl.pallas_call(
        functools.partial(attend_kernel, heads, head_size, factor),
        grid=(rows,),
        out_shape=jax.ShapeDtypeStruct((rows, width, wide), BF16),
        in_specs=[
            row_spec(width, wide),
            keys_spec(places, width, 2 * head_size),
            row_spec(width, 1),
            row_spec(width, 1),
            row_spec(1, length),
            row_spec(1, length),
        ],
        out_specs=row_spec(width, wide),
        cost_estimate=pl.CostEstimate(
            flops=4 * rows * width * wide * length,
            bytes_accessed=4 * rows * (width * wide + length * head_size),
            transcendentals=rows * width * heads * length,
        ),
        name="attend",
    )(queries, all_kv, *marks)


def attend_back(queries, d_mixed, all_kv, marks, heads, head_size, factor):
    rows, width, wide = queries.shape
    places = all_kv.shape[0]
    length = places * width
    return pl.pallas_call(
        functools.partial(attend_back_kernel, heads, head_size, factor),
        grid=(rows,),
        out_shape=(
            jax.ShapeDtypeStruct((rows, width, wide), F32),
            jax.ShapeDtypeStruct((places, rows, width, 2 * head_size), BF16),
        ),
        in_specs=[
            row_spec(width, wide),
            row_spec(width, wide),
            keys_spec(places, width, 2 * head_size),
            row_spec(width, 1),
            row_spec(width, 1),
            row_spec(1, length),
            row_spec(1, length),
        ],
        out_specs=(row_spec(width, wide), keys_spec(places, width, 2 * head_size)),
        scratch_shapes=[pltpu.VMEM((length, 2 * head_size), F32)],
        cost_estimate=pl.CostEstimate(
            flops=10 * rows * width * wide * length,
            bytes_accessed=8 * rows * (width * wide + length * head_size),
            transcendentals=rows * width * heads * length,
        ),
        name="attend_back",
    )(queries, d_mixed, all_kv, *marks)


def partners_of(core, place, head, planes, over_core):
    found = [(core, xor(place, 2 * k), head) for k in range(1, planes)]
    found.append((core, xor(place, 1), head))
    if over_core:
        found.append((1 - core, place, head))
    return found


def greet(partners):
    barrier = pltpu.get_barrier_semaphore()
    for device in partners:
        pl.semaphore_signal(barrier, inc=1, device_id=device, device_id_type=MESH)
    pl.semaphore_wait(barrier, len(partners))


def remote(source, target, send_sem, recv_sem, device):
    copy = pltpu.make_async_remote_copy(
        src_ref=source,
        dst_ref=target,
        send_sem=send_sem,
        recv_sem=recv_sem,
        device_id=device,
        device_id_type=MESH,
    )
    copy.start()
    return copy


def gather_kernel(places, flags, *refs):
    count = len(flags)
    sources, outs = refs[:count], refs[count : 2 * count]
    own_sem, send_z, recv_z, send_y, recv_y, send_c, recv_c = refs[2 * count :]
    core, place, head = lax.axis_index("dp"), lax.axis_index("seq"), lax.axis_index("head")
    planes = places // 2

    def slot(n, mask):
        where = xor(place, mask)
        return outs[n].at[core * places + where if flags[n] else where]

    greet(partners_of(core, place, head, planes, any(flags)))
    near = (core, xor(place, 1), head)
    other = (1 - core, place, head)
    along, across, over = {}, {}, {}
    for n in range(count):
        for k in range(1, planes):
            along[n, k] = remote(
                sources[n],
                slot(n, 0),
                send_z.at[n, k],
                recv_z.at[n, k],
                (core, xor(place, 2 * k), head),
            )
    local = []
    for n in range(count):
        across[n, 0] = remote(
            sources[n], slot(n, 0), send_y.at[n, 0], recv_y.at[n, 0], near
        )
        if flags[n]:
            over[n, 0] = remote(
                sources[n], slot(n, 0), send_c.at[n, 0], recv_c.at[n, 0], other
            )
        copy = pltpu.make_async_copy(sources[n], slot(n, 0), own_sem.at[n])
        copy.start()
        local.append(copy)
    for n in range(count):
        for k in range(1, planes):
            along[n, k].wait_recv()
            piece = slot(n, 2 * k)
            across[n, k] = remote(piece, piece, send_y.at[n, k], recv_y.at[n, k], near)
            if flags[n]:
                over[n, 2 * k] = remote(
                    piece, piece, send_c.at[n, 2 * k], recv_c.at[n, 2 * k], other
                )
    for n in range(count):
        for k in range(planes):
            across[n, k].wait_recv()
            if flags[n]:
                mask = 2 * k + 1
                piece = slot(n, mask)
                over[n, mask] = remote(
                    piece, piece, send_c.at[n, mask], recv_c.at[n, mask], other
                )
    for copy in over.values():
        copy.wait_recv()
    for copies in (along, across, over):
        for copy in copies.values():
            copy.wait_send()
    for copy in local:
        copy.wait()


def gather_pieces(pieces, flags, ident, name):
    places = lax.axis_size("seq")
    planes = places // 2
    count = len(pieces)
    return pl.pallas_call(
        functools.partial(gather_kernel, places, flags),
        out_shape=tuple(
            jax.ShapeDtypeStruct(((1 + flag) * places,) + piece.shape, piece.dtype)
            for piece, flag in zip(pieces, flags)
        ),
        in_specs=[pl.BlockSpec(memory_space=pltpu.VMEM)] * count,
        out_specs=tuple([pl.BlockSpec(memory_space=pl.ANY)] * count),
        scratch_shapes=[
            pltpu.SemaphoreType.DMA((count,)),
            pltpu.SemaphoreType.DMA((count, planes)),
            pltpu.SemaphoreType.DMA((count, planes)),
            pltpu.SemaphoreType.DMA((count, planes)),
            pltpu.SemaphoreType.DMA((count, planes)),
            pltpu.SemaphoreType.DMA((count, places)),
            pltpu.SemaphoreType.DMA((count, places)),
        ],
        compiler_params=pltpu.CompilerParams(collective_id=ident, has_side_effects=True),
        cost_estimate=pl.CostEstimate(flops=0, bytes_accessed=150_000_000, transcendentals=0),
        name=name,
    )(*pieces)


def reduce_kernel(places, flags, vector, *refs):
    count = len(flags)
    planes = places // 2
    step = count + vector
    grads, totals = refs[:step], refs[step : 2 * step]
    refs = refs[2 * step :]
    sems, refs = refs[:6], refs[6:]
    send_c, recv_c, send_y, recv_y, send_z, recv_z = sems
    got_c, got_y, got_z, out_y, out_z = (refs[i * step : (i + 1) * step] for i in range(5))
    core, place, head = lax.axis_index("dp"), lax.axis_index("seq"), lax.axis_index("head")
    greet(partners_of(core, place, head, planes, any(flags)))
    near = (core, xor(place, 1), head)
    other = (1 - core, place, head)
    over, across, along = {}, {}, {}
    order = [2 * k + 1 for k in range(planes)] + [2 * k for k in range(1, planes)] + [0]

    if vector:
        over[count, 0] = remote(
            grads[count], got_c[count], send_c.at[count, 0], recv_c.at[count, 0], other
        )
    for n in range(count):
        if flags[n]:
            for mask in order:
                over[n, mask] = remote(
                    grads[n].at[(1 - core) * places + xor(place, mask)],
                    got_c[n].at[mask],
                    send_c.at[n, mask],
                    recv_c.at[n, mask],
                    other,
                )

    def chip_sum(n, mask):
        where = xor(place, mask)
        if not flags[n]:
            return grads[n][where].astype(F32)
        over[n, mask].wait_recv()
        return grads[n][core * places + where].astype(F32) + got_c[n][mask].astype(F32)

    if vector:
        over[count, 0].wait_recv()
        out_y[count][...] = grads[count][...] + got_c[count][...]
        across[count, 0] = remote(
            out_y[count], got_y[count], send_y.at[count, 0], recv_y.at[count, 0], near
        )
    for n in range(count):
        for k in list(range(1, planes)) + [0]:
            out_y[n][k] = chip_sum(n, 2 * k + 1).astype(BF16)
            across[n, k] = remote(
                out_y[n].at[k], got_y[n].at[k], send_y.at[n, k], recv_y.at[n, k], near
            )
    if vector:
        across[count, 0].wait_recv()
        out_z[count][...] = out_y[count][...] + got_y[count][...]
        for k in range(1, planes):
            along[count, k] = remote(
                out_z[count],
                got_z[count].at[k],
                send_z.at[count, k],
                recv_z.at[count, k],
                (core, xor(place, 2 * k), head),
            )
    for n in range(count):
        for k in range(1, planes):
            part = chip_sum(n, 2 * k)
            across[n, k].wait_recv()
            out_z[n][k] = (part + got_y[n][k].astype(F32)).astype(BF16)
            along[n, k] = remote(
                out_z[n].at[k],
                got_z[n].at[k],
                send_z.at[n, k],
                recv_z.at[n, k],
                (core, xor(place, 2 * k), head),
            )
    for n in range(count):
        part = chip_sum(n, 0)
        across[n, 0].wait_recv()
        totals[n][...] = part + got_y[n][0].astype(F32)
    if vector:
        totals[count][...] = out_z[count][...]
    for n in range(step):
        for k in range(1, planes):
            along[n, k].wait_recv()
            totals[n][...] += got_z[n][k].astype(F32)
    for copies in (over, across, along):
        for copy in copies.values():
            copy.wait_send()


def reduce_pieces(grads, flags, vector, ident, name):
    places = lax.axis_size("seq")
    planes = places // 2
    count = len(grads)
    shapes = [grad.shape[1:] for grad in grads]
    operands = list(grads)
    step = count
    if vector is not None:
        operands.append(vector)
        step += 1
    small = (8, LANES)

    def buffers(leading, vector_leading):
        out = [pltpu.VMEM(leading + shape, BF16) for shape in shapes]
        if vector is not None:
            out.append(pltpu.VMEM(vector_leading + vector.shape, F32))
        return out

    got_c = [
        pltpu.VMEM(((places,) + shape) if flag else small, BF16)
        for shape, flag in zip(shapes, flags)
    ]
    if vector is not None:
        got_c.append(pltpu.VMEM(vector.shape, F32))
    scratch = (
        [
            pltpu.SemaphoreType.DMA((step, places)),
            pltpu.SemaphoreType.DMA((step, places)),
            pltpu.SemaphoreType.DMA((step, planes)),
            pltpu.SemaphoreType.DMA((step, planes)),
            pltpu.SemaphoreType.DMA((step, planes)),
            pltpu.SemaphoreType.DMA((step, planes)),
        ]
        + got_c
        + buffers((planes,), ())
        + buffers((planes,), (planes,))
        + buffers((planes,), ())
        + buffers((planes,), ())
    )
    out_shapes = [jax.ShapeDtypeStruct(shape, F32) for shape in shapes]
    if vector is not None:
        out_shapes.append(jax.ShapeDtypeStruct(vector.shape, F32))
    return pl.pallas_call(
        functools.partial(reduce_kernel, places, flags, int(vector is not None)),
        out_shape=tuple(out_shapes),
        in_specs=[pl.BlockSpec(memory_space=pltpu.VMEM)] * step,
        out_specs=tuple([pl.BlockSpec(memory_space=pltpu.VMEM)] * step),
        scratch_shapes=scratch,
        compiler_params=pltpu.CompilerParams(collective_id=ident, has_side_effects=True),
        cost_estimate=pl.CostEstimate(flops=0, bytes_accessed=150_000_000, transcendentals=0),
        name=name,
    )(*operands)


def join_kernel(places, count, *refs):
    pieces, out, held, in_sem, out_sem = refs[:count], *refs[count:]
    core, place = lax.axis_index("dp"), lax.axis_index("seq")
    arriving = []
    for p in range(count):
        for q in range(4):
            i = 4 * p + q
            copy = pltpu.make_async_copy(pieces[p].at[q], held.at[i], in_sem.at[i])
            copy.start()
            arriving.append(copy)
    leaving = []
    for p in range(count):
        for q in range(4):
            i = 4 * p + q
            arriving[i].wait()
            mask = 4 * (p // 2) + 2 * (q // 2) + p % 2
            where = (core if q % 2 == 0 else 1 - core) * places + xor(place, mask)
            copy = pltpu.make_async_copy(held.at[i], out.at[where], out_sem.at[i])
            copy.start()
            leaving.append(copy)
    for copy in leaving:
        copy.wait()


def join_pieces(pieces):
    places = lax.axis_size("seq")
    count = len(pieces)
    _, rows, columns = pieces[0].shape
    total = 4 * count
    out = pl.pallas_call(
        functools.partial(join_kernel, places, count),
        out_shape=jax.ShapeDtypeStruct((total, rows, columns), BF16),
        in_specs=[pl.BlockSpec(memory_space=pl.ANY)] * count,
        out_specs=pl.BlockSpec(memory_space=pl.ANY),
        scratch_shapes=[
            pltpu.VMEM((total, rows, columns), BF16),
            pltpu.SemaphoreType.DMA((total,)),
            pltpu.SemaphoreType.DMA((total,)),
        ],
        cost_estimate=pl.CostEstimate(
            flops=0, bytes_accessed=4 * total * rows * columns, transcendentals=0
        ),
        name="join",
    )(*pieces)
    return out.reshape(total * rows, columns)


def place_kernel(units, block, turn, *refs):
    pieces, out, held = refs[:4], refs[4], refs[5]
    core, place = lax.axis_index("dp"), lax.axis_index("seq")
    for q in range(4):
        where = xor(lax.rem(lax.div(place, 2), 2) * 2 + core, q)
        columns = pl.ds(pl.multiple_of(where * block, LANES), block)
        held[:, columns] = pieces[q][...].astype(F32)
    whole = held[:, :units]
    out[...] = whole.T if turn else whole


def place_pieces(pieces, units, turn):
    rows, block = pieces[0].shape
    shape = (units, rows) if turn else (rows, units)
    return pl.pallas_call(
        functools.partial(place_kernel, units, block, turn),
        out_shape=jax.ShapeDtypeStruct(shape, F32),
        in_specs=[pl.BlockSpec(memory_space=pltpu.VMEM)] * 4,
        out_specs=pl.BlockSpec(memory_space=pltpu.VMEM),
        scratch_shapes=[pltpu.VMEM((rows, 4 * block), F32)],
        cost_estimate=pl.CostEstimate(
            flops=0, bytes_accessed=8 * rows * units, transcendentals=0
        ),
        name="place",
    )(*pieces)


def sum_heads(part):
    low = lax.reduce_precision(part, 8, 7).astype(BF16)
    return low.astype(F32) + flip(low, "head", 1).astype(F32)


def spread_tokens(values):
    far = flip(values, "seq", 2)
    return jnp.concatenate([values, flip(values, "dp", 1), far, flip(far, "dp", 1)], axis=0)


def collect_tokens(part):
    blocks = part.reshape((2, 2, -1) + part.shape[1:])
    far = flip(blocks[1].astype(BF16), "seq", 2)
    both = blocks[0].astype(F32) + far.astype(F32)
    return both[0] + flip(both[1].astype(BF16), "dp", 1).astype(F32)


def in_order(own, other, head, axis):
    first = head == 0
    return jnp.concatenate(
        [jnp.where(first, own, other), jnp.where(first, other, own)], axis=axis
    )


def on_device(
    hidden_in,
    segment_ids,
    position_ids,
    out_cot,
    attn_gain,
    w_query,
    b_query,
    w_key,
    b_key,
    w_value,
    b_value,
    w_out,
    ffn_gain,
    w_gate,
    w_up,
    w_down,
):
    row_count, row_width, model_width = hidden_in.shape
    tokens = row_count * row_width
    heads, head_size = b_query.shape
    wide = heads * head_size
    factor = head_size ** (-0.5)
    places = lax.axis_size("seq")
    columns = places // 4
    core = lax.axis_index("dp")
    place = lax.axis_index("seq")
    head = lax.axis_index("head")
    column = place // 4
    level = (place // 2) % 2
    side = place % 2
    shard = w_gate.shape[0]
    units = w_gate.shape[1]
    block = -(-units // (4 * LANES)) * LANES

    here = level * 2 + core
    stacked = jnp.stack([w_gate, w_up, w_down.T])
    stacked = jnp.pad(stacked, ((0, 0), (0, 0), (0, 4 * block - units)))
    quarters = []
    for m in range(4):
        piece = lax.dynamic_slice_in_dim(stacked, (here ^ m) * block, block, 2)
        quarters.append(flip_pair(piece, m % 2, m // 2 * 2) if m else piece)

    marks_own = jnp.concatenate([segment_ids, position_ids], axis=0)
    full_qkv, full_out, marks_all = gather_pieces(
        [jnp.concatenate([w_query, w_key, w_value], axis=1), w_out.T, marks_own],
        (1, 1, 0),
        0,
        "gather_weights",
    )
    full_qkv = full_qkv.reshape(model_width, -1)
    full_out = full_out.reshape(model_width, -1)
    marks_all = marks_all.reshape(places, 2, row_count, row_width).transpose(1, 2, 0, 3)
    marks_all = marks_all.reshape(2, row_count, 1, places * row_width)
    marks = (
        segment_ids[:, :, None],
        position_ids[:, :, None],
        marks_all[0],
        marks_all[1],
    )

    near_weights = [jnp.stack([quarter[i] for quarter in quarters]) for i in range(3)]

    def column_gather(own):
        return [own] + [flip(own, "seq", 4 * k) for k in range(1, columns)]

    gate_parts = column_gather(after(near_weights[0], full_qkv))

    hidden = hidden_in.reshape(tokens, model_width).astype(F32)
    scale_one = norm_scale(hidden)
    gain_one = attn_gain.astype(F32)
    normed = (hidden * scale_one * gain_one).astype(BF16)
    cosine, sine_table = rope_tables(position_ids.reshape(tokens), head_size)
    bias = jnp.concatenate([b_query.reshape(-1), b_key.reshape(-1), b_value.reshape(-1)])
    qkv = plain_dot(normed, full_qkv) + bias.astype(F32)
    queries = rotate(
        qkv[:, :wide].reshape(tokens, heads, head_size),
        cosine[:, None, :],
        sine_table[:, None, :],
        1.0,
    ).astype(BF16)
    queries = queries.reshape(row_count, row_width, wide)
    key_rot = rotate(qkv[:, wide : wide + head_size], cosine, sine_table, 1.0).astype(BF16)
    local_kv = jnp.concatenate([key_rot, qkv[:, wide + head_size :].astype(BF16)], axis=-1)
    local_kv = local_kv.reshape(row_count, row_width, 2 * head_size)
    (all_kv,) = gather_pieces([local_kv], (0,), 1, "gather_keys")

    up_parts = column_gather(after(near_weights[1], all_kv))
    down_parts = column_gather(after(near_weights[2], all_kv))

    def side_gather(parts):
        pieces = []
        for part in parts:
            pieces += [part, flip(part, "seq", 1)]
        return join_pieces(pieces)

    full_gate = side_gather([after(part, all_kv) for part in gate_parts])
    full_up = side_gather(up_parts)
    full_down = side_gather(down_parts)

    out_other = flip(after(full_out, all_kv), "head", 1)
    out_all = in_order(full_out, out_other, head, 1)

    live_rows = (segment_ids != 0).astype(F32).reshape(tokens, 1)
    cotangent = out_cot.reshape(tokens, model_width).astype(F32) * live_rows
    cot_low = spread_tokens(after(cotangent.astype(BF16), all_kv))

    mixed = attend(queries, all_kv, marks, heads, head_size, factor).reshape(tokens, wide)
    mixed_all = in_order(mixed, flip(mixed, "head", 1), head, 1)
    middle = hidden + through_weight(mixed_all, out_all)
    scale_two = norm_scale(middle)
    gain_two = ffn_gain.astype(F32)
    normed_two = spread_tokens((middle * scale_two * gain_two).astype(BF16))

    gate_pre = plain_dot(normed_two, full_gate)
    up_pre = plain_dot(normed_two, full_up)
    sigmoid_gate = jax.nn.sigmoid(gate_pre)
    activated = gate_pre * sigmoid_gate
    product = (activated * up_pre).astype(BF16)
    d_product = plain_dot(cot_low, full_down).astype(BF16).astype(F32)
    d_gate = (d_product * up_pre * sigmoid_gate * (1.0 + gate_pre * (1.0 - sigmoid_gate))).astype(
        BF16
    )
    d_up = (d_product * activated).astype(BF16)
    back_two = through_weight(d_gate, full_gate) + through_weight(d_up, full_up)
    back_two = sum_heads(collect_tokens(back_two))
    grad_down = grad_of_weight(cot_low, product).astype(BF16)
    grad_gate = grad_of_weight(normed_two, d_gate).astype(BF16)
    grad_up = grad_of_weight(normed_two, d_up).astype(BF16)
    result = middle + sum_heads(collect_tokens(through_weight(product, full_down)))
    layer_out = result.astype(BF16).reshape(row_count, row_width, model_width)

    ffn_sums = []
    for n, grad in enumerate((grad_down, grad_gate, grad_up)):
        blocks = grad.reshape(2, columns, 2, 2, shard, block)
        half = take(blocks, side, 3).astype(F32)
        half = half + flip(take(blocks, 1 - side, 3), "seq", 1).astype(F32)
        low = half.astype(BF16)
        total = take(half, column, 1)
        for k in range(1, columns):
            total = total + flip(take(low, column ^ k, 1), "seq", 4 * k).astype(F32)
        total = total.astype(BF16)
        pieces = []
        for m in range(4):
            piece = lax.dynamic_slice(
                total,
                (core ^ (m % 2), level ^ (m // 2), 0, 0),
                (1, 1, shard, block),
            ).reshape(shard, block)
            pieces.append(flip_pair(piece, m % 2, m // 2 * 2) if m else piece)
        ffn_sums.append(place_pieces(pieces, units, n == 0))
    down_sum, gate_sum, up_sum = ffn_sums

    gain_two_grad = jnp.sum(back_two * middle * scale_two, axis=0)
    d_middle = cotangent + norm_back(back_two, middle, scale_two, gain_two)
    d_middle_low = d_middle.astype(BF16)
    d_mixed = plain_dot(d_middle_low, full_out).astype(BF16)

    d_query, d_kv_all = attend_back(
        queries,
        d_mixed.reshape(row_count, row_width, wide),
        all_kv,
        marks,
        heads,
        head_size,
        factor,
    )
    (d_kv,) = reduce_pieces([d_kv_all], (0,), None, 2, "reduce_keys")
    d_kv = d_kv.reshape(tokens, 2 * head_size)
    d_key = rotate(d_kv[:, :head_size], cosine, sine_table, -1.0).astype(BF16)
    d_value = d_kv[:, head_size:].astype(BF16)
    d_query = rotate(
        d_query.reshape(tokens, heads, head_size),
        cosine[:, None, :],
        sine_table[:, None, :],
        -1.0,
    ).astype(BF16)
    d_qkv = jnp.concatenate([d_query.reshape(tokens, wide), d_key, d_value], axis=-1)
    back_one = sum_heads(through_weight(d_qkv, full_qkv))
    d_hidden = d_middle + norm_back(back_one, hidden, scale_one, gain_one)
    input_grad = d_hidden.astype(BF16).reshape(row_count, row_width, model_width)

    bias_grad = jnp.sum(d_qkv.astype(F32), axis=0)
    gain_one_grad = jnp.sum(back_one * hidden * scale_one, axis=0)
    vectors = jnp.concatenate([bias_grad, gain_two_grad, gain_one_grad])
    qkv_grad = grad_of_weight(normed, d_qkv).astype(BF16).reshape(2 * places, shard, -1)
    out_grad = grad_of_weight(d_middle_low, mixed).astype(BF16).reshape(2 * places, shard, -1)
    qkv_sum, out_sum, vectors = reduce_pieces(
        [qkv_grad, out_grad], (1, 1), vectors.reshape(-1, LANES), 3, "reduce_weights"
    )
    out_sum = out_sum.T
    vectors = vectors.reshape(-1)
    index = core * places + place
    replicas = 2 * places
    narrow = head_size // replicas
    bias_sums = vectors[: wide + 2 * head_size].reshape(heads + 2, head_size)
    bias_mine = lax.dynamic_slice_in_dim(bias_sums, index * narrow, narrow, 1)
    gains = vectors[wide + 2 * head_size :].reshape(2, replicas, model_width // replicas)
    gains_mine = take(gains, index, 1)
    return (
        layer_out,
        input_grad,
        gains_mine[1],
        qkv_sum[:, :wide],
        bias_mine[:heads],
        qkv_sum[:, wide : wide + head_size],
        bias_sums[heads : heads + 1],
        qkv_sum[:, wide + head_size :],
        bias_mine[heads + 1 :],
        out_sum,
        gains_mine[0],
        gate_sum,
        up_sum,
        down_sum,
    )


def solution(mesh):
    placed = (
        P("dp", "seq", None),
        P("dp", "seq"),
        P("dp", "seq"),
        P("dp", "seq", None),
        P(),
        P(("dp", "seq"), "head"),
        P("head", None),
        P(("dp", "seq"), "head"),
        P("head", None),
        P(("dp", "seq"), "head"),
        P("head", None),
        P("head", ("dp", "seq")),
        P(),
        P(("dp", "seq"), "head"),
        P(("dp", "seq"), "head"),
        P("head", ("dp", "seq")),
    )
    return jax.shard_map(
        on_device,
        mesh=mesh,
        in_specs=placed,
        out_specs=(
            P("dp", "seq", None),
            P("dp", "seq", None),
            P(("dp", "seq")),
            P(("dp", "seq"), "head"),
            P("head", ("dp", "seq")),
            P(("dp", "seq"), "head"),
            P("head", None),
            P(("dp", "seq"), "head"),
            P("head", ("dp", "seq")),
            P("head", ("dp", "seq")),
            P(("dp", "seq")),
            P(("dp", "seq"), "head"),
            P(("dp", "seq"), "head"),
            P("head", ("dp", "seq")),
        ),
        check_vma=False,
    )
```

```python
import functools

import jax
import jax.numpy as jnp
from jax import lax
from jax.experimental import pallas as pl
from jax.experimental.pallas import tpu as pltpu
from jax.sharding import PartitionSpec as P


EPSILON = 1e-06
THETA = 1000000.0
MASKED = -1e30
LANES = 128
BF16 = jnp.bfloat16
F32 = jnp.float32
MESH = pl.DeviceIdType.MESH


def rope_tables(position, head_size):
    half_size = head_size // 2
    frequency = THETA ** (-jnp.arange(half_size, dtype=F32) * 2.0 / head_size)
    angles = position.astype(F32)[:, None] * frequency[None, :]
    return jnp.cos(angles), jnp.sin(angles)


def rotate(values, cosine, sine_table, direction):
    half_size = values.shape[-1] // 2
    first_half = values[..., :half_size]
    second_half = values[..., half_size:]
    return jnp.concatenate(
        [
            first_half * cosine - direction * (second_half * sine_table),
            second_half * cosine + direction * (first_half * sine_table),
        ],
        axis=-1,
    )


def xor(index, mask):
    out = index
    bit = 1
    while bit <= mask:
        if mask & bit:
            out = out + bit - 2 * bit * lax.rem(lax.div(index, bit), 2)
        bit *= 2
    return out


def plain_dot(left, right):
    return jnp.dot(left, right, preferred_element_type=F32)


def grad_of_weight(left, right):
    return lax.dot_general(left, right, (((0,), (0,)), ((), ())), preferred_element_type=F32)


def through_weight(left, right):
    return lax.dot_general(left, right, (((1,), (1,)), ((), ())), preferred_element_type=F32)


def norm_scale(values):
    return lax.rsqrt(jnp.mean(values * values, axis=-1, keepdims=True) + EPSILON)


def norm_back(grad_in, values, scale_rows, gain):
    scaled = grad_in * gain
    cubed = scale_rows * scale_rows * scale_rows
    return scale_rows * scaled - values * cubed * jnp.mean(scaled * values, axis=-1, keepdims=True)


def flip(values, axis, mask):
    size = lax.axis_size(axis)
    return lax.ppermute(values, axis, [(i, i ^ mask) for i in range(size)])


def after(values, gate):
    return lax.optimization_barrier((values, gate))[0]


def take(buffer, index, axis=0):
    return lax.dynamic_index_in_dim(buffer, index, axis, keepdims=False)


def allowed_keys(seg_q, pos_q, seg_k, pos_k):
    return (seg_q == seg_k) & (pos_k <= pos_q)


def dot_nt(left, right):
    return lax.dot_general(left, right, (((1,), (1,)), ((), ())), preferred_element_type=F32)


def dot_tn(left, right):
    return lax.dot_general(left, right, (((0,), (0,)), ((), ())), preferred_element_type=F32)


def probabilities(query, keys, allowed, factor):
    scores = jnp.where(allowed, dot_nt(query, keys) * factor, MASKED)
    top = jnp.max(scores, axis=-1, keepdims=True)
    terms = jnp.where(allowed, jnp.exp(scores - top), 0.0)
    return terms / jnp.sum(terms, axis=-1, keepdims=True)


def attend_kernel(heads, head_size, factor, q_ref, kv_ref, sq_ref, pq_ref, sk_ref, pk_ref, o_ref):
    allowed = allowed_keys(sq_ref[0], pq_ref[0], sk_ref[0], pk_ref[0])
    joint = kv_ref[:, 0].reshape(-1, 2 * head_size)
    keys = joint[:, :head_size]
    values = joint[:, head_size:]
    for head in range(heads):
        lanes = slice(head * head_size, (head + 1) * head_size)
        probs = probabilities(q_ref[0, :, lanes], keys, allowed, factor)
        o_ref[0, :, lanes] = jnp.dot(
            probs.astype(BF16), values, preferred_element_type=F32
        ).astype(BF16)


def attend_back_kernel(
    heads, head_size, factor, q_ref, do_ref, kv_ref, sq_ref, pq_ref, sk_ref, pk_ref,
    cos_ref, sin_ref, dq_ref, dkv_ref, acc
):
    allowed = allowed_keys(sq_ref[0], pq_ref[0], sk_ref[0], pk_ref[0])
    joint = kv_ref[:, 0].reshape(-1, 2 * head_size)
    keys = joint[:, :head_size]
    values = joint[:, head_size:]
    for head in range(heads):
        lanes = slice(head * head_size, (head + 1) * head_size)
        query = q_ref[0, :, lanes]
        d_out = do_ref[0, :, lanes]
        probs = probabilities(query, keys, allowed, factor)
        d_probs = dot_nt(d_out, values)
        delta = jnp.sum(probs * d_probs, axis=-1, keepdims=True)
        d_scores = (probs * (d_probs - delta)).astype(BF16)
        d_query = jnp.dot(d_scores, keys, preferred_element_type=F32) * factor
        turned = pltpu.roll(d_query, head_size // 2, 1)
        dq_ref[0, :, lanes] = (d_query * cos_ref[0] + turned * sin_ref[0]).astype(BF16)
        d_key = dot_tn(d_scores, query) * factor
        d_value = dot_tn(probs.astype(BF16), d_out)
        if head == 0:
            acc[:, :head_size] = d_key
            acc[:, head_size:] = d_value
        else:
            acc[:, :head_size] += d_key
            acc[:, head_size:] += d_value
    dkv_ref[:, 0] = acc[...].astype(BF16).reshape(dkv_ref.shape[0], -1, 2 * head_size)


def row_spec(*shape):
    return pl.BlockSpec((1,) + shape, lambda row: (row,) + (0,) * len(shape))


def keys_spec(places, *shape):
    return pl.BlockSpec(
        (places, 1) + shape, lambda row: (0, row) + (0,) * len(shape)
    )


def attend(queries, all_kv, marks, heads, head_size, factor):
    rows, width, wide = queries.shape
    places = all_kv.shape[0]
    length = places * width
    return pl.pallas_call(
        functools.partial(attend_kernel, heads, head_size, factor),
        grid=(rows,),
        out_shape=jax.ShapeDtypeStruct((rows, width, wide), BF16),
        in_specs=[
            row_spec(width, wide),
            keys_spec(places, width, 2 * head_size),
            row_spec(width, 1),
            row_spec(width, 1),
            row_spec(1, length),
            row_spec(1, length),
        ],
        out_specs=row_spec(width, wide),
        cost_estimate=pl.CostEstimate(
            flops=4 * rows * width * wide * length,
            bytes_accessed=4 * rows * (width * wide + length * head_size),
            transcendentals=rows * width * heads * length,
        ),
        name="attend",
    )(queries, all_kv, *marks)


def attend_back(queries, d_mixed, all_kv, marks, turns, heads, head_size, factor):
    rows, width, wide = queries.shape
    places = all_kv.shape[0]
    length = places * width
    return pl.pallas_call(
        functools.partial(attend_back_kernel, heads, head_size, factor),
        grid=(rows,),
        out_shape=(
            jax.ShapeDtypeStruct((rows, width, wide), BF16),
            jax.ShapeDtypeStruct((places, rows, width, 2 * head_size), BF16),
        ),
        in_specs=[
            row_spec(width, wide),
            row_spec(width, wide),
            keys_spec(places, width, 2 * head_size),
            row_spec(width, 1),
            row_spec(width, 1),
            row_spec(1, length),
            row_spec(1, length),
            row_spec(width, head_size),
            row_spec(width, head_size),
        ],
        out_specs=(row_spec(width, wide), keys_spec(places, width, 2 * head_size)),
        scratch_shapes=[pltpu.VMEM((length, 2 * head_size), F32)],
        cost_estimate=pl.CostEstimate(
            flops=10 * rows * width * wide * length,
            bytes_accessed=8 * rows * (width * wide + length * head_size),
            transcendentals=rows * width * heads * length,
        ),
        name="attend_back",
    )(queries, d_mixed, all_kv, *marks, *turns)


def partners_of(core, place, head, planes, over_core):
    found = [(core, xor(place, 2 * k), head) for k in range(1, planes)]
    found.append((core, xor(place, 1), head))
    if over_core:
        found.append((1 - core, place, head))
    return found


def greet(partners):
    barrier = pltpu.get_barrier_semaphore()
    for device in partners:
        pl.semaphore_signal(barrier, inc=1, device_id=device, device_id_type=MESH)
    pl.semaphore_wait(barrier, len(partners))


def remote(source, target, send_sem, recv_sem, device):
    copy = pltpu.make_async_remote_copy(
        src_ref=source,
        dst_ref=target,
        send_sem=send_sem,
        recv_sem=recv_sem,
        device_id=device,
        device_id_type=MESH,
    )
    copy.start()
    return copy


def quarter_start(which, block, units):
    return pl.multiple_of(which * block - lax.div(which, 3) * (4 * block - units), LANES)


def gather_kernel(places, flags, extra, block, normed, *refs):
    count = len(flags)
    sources, refs = refs[:count], refs[count:]
    weights, refs = refs[:extra], refs[extra:]
    if normed:
        (hidden_ref, gain_ref), refs = refs[:2], refs[2:]
    outs, refs = refs[:count], refs[count:]
    nears, refs = refs[:extra], refs[extra:]
    if normed:
        normed_ref, refs = refs[0], refs[1:]
    own_sem, send_z, recv_z, send_y, recv_y, send_c, recv_c, send_q, recv_q = refs
    core, place, head = lax.axis_index("dp"), lax.axis_index("seq"), lax.axis_index("head")
    planes = places // 2

    def slot(n, mask):
        where = xor(place, mask)
        return outs[n].at[core * places + where if flags[n] else where]

    partners = partners_of(core, place, head, planes, any(flags))
    if extra:
        partners.append((1 - core, xor(place, 2), head))
    greet(partners)
    near = (core, xor(place, 1), head)
    other = (1 - core, place, head)
    along, across, over, quarter = {}, {}, {}, {}
    for n in range(count):
        for k in range(1, planes):
            along[n, k] = remote(
                sources[n],
                slot(n, 0),
                send_z.at[n, k],
                recv_z.at[n, k],
                (core, xor(place, 2 * k), head),
            )
    local = []
    for n in range(count):
        across[n, 0] = remote(
            sources[n], slot(n, 0), send_y.at[n, 0], recv_y.at[n, 0], near
        )
        if flags[n]:
            over[n, 0] = remote(
                sources[n], slot(n, 0), send_c.at[n, 0], recv_c.at[n, 0], other
            )
        copy = pltpu.make_async_copy(sources[n], slot(n, 0), own_sem.at[n])
        copy.start()
        local.append(copy)
    for n in range(extra):
        units = weights[n].shape[1]
        for m in range(4):
            to_core = core if m % 2 == 0 else 1 - core
            to_place = xor(place, m // 2 * 2)
            which = lax.rem(lax.div(to_place, 2), 2) * 2 + to_core
            piece = weights[n].at[:, pl.ds(quarter_start(which, block, units), block)]
            if m:
                quarter[n, m] = remote(
                    piece,
                    nears[n].at[m],
                    send_q.at[n, m],
                    recv_q.at[n, m],
                    (to_core, to_place, head),
                )
            else:
                copy = pltpu.make_async_copy(piece, nears[n].at[0], send_q.at[n, 0])
                copy.start()
                local.append(copy)
    if normed:
        for row in range(hidden_ref.shape[0]):
            values = hidden_ref[row].astype(F32)
            normed_ref[row] = (values * norm_scale(values) * gain_ref[...]).astype(BF16)
    for n in range(count):
        for k in range(1, planes):
            along[n, k].wait_recv()
            piece = slot(n, 2 * k)
            across[n, k] = remote(piece, piece, send_y.at[n, k], recv_y.at[n, k], near)
            if flags[n]:
                over[n, 2 * k] = remote(
                    piece, piece, send_c.at[n, 2 * k], recv_c.at[n, 2 * k], other
                )
    for n in range(count):
        for k in range(planes):
            across[n, k].wait_recv()
            if flags[n]:
                mask = 2 * k + 1
                piece = slot(n, mask)
                over[n, mask] = remote(
                    piece, piece, send_c.at[n, mask], recv_c.at[n, mask], other
                )
    for copies in (over, quarter):
        for copy in copies.values():
            copy.wait_recv()
    for copies in (along, across, over, quarter):
        for copy in copies.values():
            copy.wait_send()
    for copy in local:
        copy.wait()


def gather_pieces(pieces, flags, ident, weights=(), block=0, norm=None):
    places = lax.axis_size("seq")
    planes = places // 2
    count, extra = len(pieces), len(weights)
    out_shape = [
        jax.ShapeDtypeStruct(((1 + flag) * places,) + piece.shape, piece.dtype)
        for piece, flag in zip(pieces, flags)
    ]
    out_shape += [jax.ShapeDtypeStruct((4, w.shape[0], block), w.dtype) for w in weights]
    out_specs = [pl.BlockSpec(memory_space=pl.ANY)] * (count + extra)
    operands = list(pieces) + list(weights)
    if norm is not None:
        operands += list(norm)
        out_shape.append(jax.ShapeDtypeStruct(norm[0].shape, BF16))
        out_specs.append(pl.BlockSpec(memory_space=pltpu.VMEM))
    quarters = (max(extra, 1), 4)
    return pl.pallas_call(
        functools.partial(gather_kernel, places, flags, extra, block, norm is not None),
        out_shape=tuple(out_shape),
        in_specs=[pl.BlockSpec(memory_space=pltpu.VMEM)] * len(operands),
        out_specs=tuple(out_specs),
        scratch_shapes=[
            pltpu.SemaphoreType.DMA((count,)),
            pltpu.SemaphoreType.DMA((count, planes)),
            pltpu.SemaphoreType.DMA((count, planes)),
            pltpu.SemaphoreType.DMA((count, planes)),
            pltpu.SemaphoreType.DMA((count, planes)),
            pltpu.SemaphoreType.DMA((count, places)),
            pltpu.SemaphoreType.DMA((count, places)),
            pltpu.SemaphoreType.DMA(quarters),
            pltpu.SemaphoreType.DMA(quarters),
        ],
        compiler_params=pltpu.CompilerParams(collective_id=ident, has_side_effects=True),
        cost_estimate=pl.CostEstimate(flops=0, bytes_accessed=100_000_000, transcendentals=0),
    )(*operands)


def reduce_kernel(places, flags, vector, first_row, extra, block, *refs):
    count = len(flags)
    planes = places // 2
    step = count + vector
    grads, refs = refs[:step], refs[step:]
    pieces, refs = refs[:extra], refs[extra:]
    totals, refs = refs[:step], refs[step:]
    wholes, refs = refs[:extra], refs[extra:]
    sems, refs = refs[:8], refs[8:]
    send_c, recv_c, send_y, recv_y, send_z, recv_z, send_q, recv_q = sems
    got_c, got_y, got_z, out_y, out_z = (refs[i * step : (i + 1) * step] for i in range(5))
    refs = refs[5 * step :]
    got_q, refs = refs[:extra], refs[extra:]
    core, place, head = lax.axis_index("dp"), lax.axis_index("seq"), lax.axis_index("head")
    level = lax.rem(lax.div(place, 2), 2)
    partners = partners_of(core, place, head, planes, any(flags))
    if extra:
        partners.append((1 - core, xor(place, 2), head))
    if vector:
        partners.append((core, place, 1 - head))
    greet(partners)
    near = (core, xor(place, 1), head)
    other = (1 - core, place, head)
    over, across, along, quarter = {}, {}, {}, {}
    order = [2 * k + 1 for k in range(planes)] + [2 * k for k in range(1, planes)] + [0]

    if vector:
        got_x, sum_x, sem_x = refs
        facing = remote(
            grads[count], got_x, sem_x.at[0], sem_x.at[1], (core, place, 1 - head)
        )
    for n in range(count):
        if flags[n]:
            for mask in order:
                over[n, mask] = remote(
                    grads[n].at[(1 - core) * places + xor(place, mask)],
                    got_c[n].at[mask],
                    send_c.at[n, mask],
                    recv_c.at[n, mask],
                    other,
                )
    for n in range(extra):
        for m in range(1, 4):
            to_core = core if m % 2 == 0 else 1 - core
            to_place = xor(place, m // 2 * 2)
            quarter[n, m] = remote(
                pieces[n].at[to_core, lax.rem(lax.div(to_place, 2), 2)],
                got_q[n].at[m],
                send_q.at[n, m],
                recv_q.at[n, m],
                (to_core, to_place, head),
            )

    def chip_sum(n, mask):
        where = xor(place, mask)
        if not flags[n]:
            return grads[n][where].astype(F32)
        over[n, mask].wait_recv()
        return grads[n][core * places + where].astype(F32) + got_c[n][mask].astype(F32)

    if vector:
        facing.wait_recv()
        rows = lax.broadcasted_iota(jnp.int32, got_x.shape, 0)
        sum_x[...] = grads[count][...] + jnp.where(rows >= first_row, got_x[...], 0.0)
        over[count, 0] = remote(
            sum_x, got_c[count], send_c.at[count, 0], recv_c.at[count, 0], other
        )
    for n in range(count):
        for k in list(range(1, planes)) + [0]:
            out_y[n][k] = chip_sum(n, 2 * k + 1).astype(BF16)
            across[n, k] = remote(
                out_y[n].at[k], got_y[n].at[k], send_y.at[n, k], recv_y.at[n, k], near
            )
    if vector:
        over[count, 0].wait_recv()
        out_y[count][...] = sum_x[...] + got_c[count][...]
        across[count, 0] = remote(
            out_y[count], got_y[count], send_y.at[count, 0], recv_y.at[count, 0], near
        )
    for n in range(extra):
        wholes[n][...] = jnp.zeros_like(wholes[n])
        units = wholes[n].shape[1]
        columns = pl.ds(quarter_start(level * 2 + core, block, units), block)
        wholes[n][:, columns] += pieces[n][core, level].astype(F32)
    for n in range(count):
        for k in range(1, planes):
            part = chip_sum(n, 2 * k)
            across[n, k].wait_recv()
            out_z[n][k] = (part + got_y[n][k].astype(F32)).astype(BF16)
            along[n, k] = remote(
                out_z[n].at[k],
                got_z[n].at[k],
                send_z.at[n, k],
                recv_z.at[n, k],
                (core, xor(place, 2 * k), head),
            )
    if vector:
        across[count, 0].wait_recv()
        out_z[count][...] = out_y[count][...] + got_y[count][...]
        for k in range(1, planes):
            along[count, k] = remote(
                out_z[count],
                got_z[count].at[k],
                send_z.at[count, k],
                recv_z.at[count, k],
                (core, xor(place, 2 * k), head),
            )
    for n in range(extra):
        units = wholes[n].shape[1]
        for m in range(1, 4):
            to_core = core if m % 2 == 0 else 1 - core
            which = (level if m < 2 else 1 - level) * 2 + to_core
            quarter[n, m].wait_recv()
            columns = pl.ds(quarter_start(which, block, units), block)
            wholes[n][:, columns] += got_q[n][m].astype(F32)
    for n in range(count):
        part = chip_sum(n, 0)
        across[n, 0].wait_recv()
        totals[n][...] = part + got_y[n][0].astype(F32)
    if vector:
        totals[count][...] = out_z[count][...]
    for n in range(step):
        for k in range(1, planes):
            along[n, k].wait_recv()
            totals[n][...] += got_z[n][k].astype(F32)
    if vector:
        facing.wait_send()
    for copies in (over, across, along, quarter):
        for copy in copies.values():
            copy.wait_send()


def reduce_pieces(grads, flags, vector, ident, first_row=0, pieces=(), units=0):
    places = lax.axis_size("seq")
    planes = places // 2
    count, extra = len(grads), len(pieces)
    shapes = [grad.shape[1:] for grad in grads]
    operands = list(grads)
    step = count
    if vector is not None:
        operands.append(vector)
        step += 1
    operands += list(pieces)
    block = pieces[0].shape[-1] if extra else 0
    small = (8, LANES)

    def buffers(leading, vector_leading):
        out = [pltpu.VMEM(leading + shape, BF16) for shape in shapes]
        if vector is not None:
            out.append(pltpu.VMEM(vector_leading + vector.shape, F32))
        return out

    got_c = [
        pltpu.VMEM(((places,) + shape) if flag else small, BF16)
        for shape, flag in zip(shapes, flags)
    ]
    if vector is not None:
        got_c.append(pltpu.VMEM(vector.shape, F32))
    quarters = (max(extra, 1), 4)
    scratch = (
        [
            pltpu.SemaphoreType.DMA((step, places)),
            pltpu.SemaphoreType.DMA((step, places)),
            pltpu.SemaphoreType.DMA((step, planes)),
            pltpu.SemaphoreType.DMA((step, planes)),
            pltpu.SemaphoreType.DMA((step, planes)),
            pltpu.SemaphoreType.DMA((step, planes)),
            pltpu.SemaphoreType.DMA(quarters),
            pltpu.SemaphoreType.DMA(quarters),
        ]
        + got_c
        + buffers((planes,), ())
        + buffers((planes,), (planes,))
        + buffers((planes,), ())
        + buffers((planes,), ())
        + [pltpu.VMEM((4,) + piece.shape[2:], BF16) for piece in pieces]
    )
    out_shapes = [jax.ShapeDtypeStruct(shape, F32) for shape in shapes]
    if vector is not None:
        scratch += [
            pltpu.VMEM(vector.shape, F32),
            pltpu.VMEM(vector.shape, F32),
            pltpu.SemaphoreType.DMA((2,)),
        ]
        out_shapes.append(jax.ShapeDtypeStruct(vector.shape, F32))
    out_shapes += [jax.ShapeDtypeStruct((piece.shape[2], units), F32) for piece in pieces]
    return pl.pallas_call(
        functools.partial(
            reduce_kernel, places, flags, int(vector is not None), first_row, extra, block
        ),
        out_shape=tuple(out_shapes),
        in_specs=[pl.BlockSpec(memory_space=pltpu.VMEM)] * len(operands),
        out_specs=tuple([pl.BlockSpec(memory_space=pltpu.VMEM)] * len(out_shapes)),
        scratch_shapes=scratch,
        compiler_params=pltpu.CompilerParams(collective_id=ident, has_side_effects=True),
        cost_estimate=pl.CostEstimate(flops=0, bytes_accessed=100_000_000, transcendentals=0),
    )(*operands)


def join_kernel(places, count, *refs):
    pieces, out, held, in_sem, out_sem = refs[:count], *refs[count:]
    core, place = lax.axis_index("dp"), lax.axis_index("seq")
    arriving = []
    for p in range(count):
        for q in range(4):
            i = 4 * p + q
            copy = pltpu.make_async_copy(pieces[p].at[q], held.at[i], in_sem.at[i])
            copy.start()
            arriving.append(copy)
    leaving = []
    for p in range(count):
        for q in range(4):
            i = 4 * p + q
            arriving[i].wait()
            mask = 4 * (p // 2) + 2 * (q // 2) + p % 2
            where = (core if q % 2 == 0 else 1 - core) * places + xor(place, mask)
            copy = pltpu.make_async_copy(held.at[i], out.at[where], out_sem.at[i])
            copy.start()
            leaving.append(copy)
    for copy in leaving:
        copy.wait()


def join_pieces(pieces):
    places = lax.axis_size("seq")
    count = len(pieces)
    _, rows, columns = pieces[0].shape
    total = 4 * count
    out = pl.pallas_call(
        functools.partial(join_kernel, places, count),
        out_shape=jax.ShapeDtypeStruct((total, rows, columns), BF16),
        in_specs=[pl.BlockSpec(memory_space=pl.ANY)] * count,
        out_specs=pl.BlockSpec(memory_space=pl.ANY),
        scratch_shapes=[
            pltpu.VMEM((total, rows, columns), BF16),
            pltpu.SemaphoreType.DMA((total,)),
            pltpu.SemaphoreType.DMA((total,)),
        ],
        cost_estimate=pl.CostEstimate(
            flops=0, bytes_accessed=4 * total * rows * columns, transcendentals=0
        ),
        name="join",
    )(*pieces)
    return out.reshape(total * rows, columns)


def sum_heads(part):
    low = lax.reduce_precision(part, 8, 7).astype(BF16)
    return low.astype(F32) + flip(low, "head", 1).astype(F32)


def in_order(own, other, head, axis):
    first = head == 0
    return jnp.concatenate(
        [jnp.where(first, own, other), jnp.where(first, other, own)], axis=axis
    )


def both_cores(values):
    return jnp.concatenate([values, flip(values, "dp", 1)], axis=0)


def far_rows(values, head):
    half = values.shape[0] // 2
    got = flip(lax.dynamic_slice_in_dim(values, head * half, half, 0), "seq", 2)
    return in_order(got, flip(got, "head", 1), head, 0)


def core_sum(part):
    half = part.shape[0] // 2
    return part[:half] + flip(part[half:].astype(BF16), "dp", 1).astype(F32)


def collect(near, far, pieces):
    far_low = core_sum(far).astype(BF16)
    near = core_sum(near)
    size = near.shape[0] // pieces
    out = []
    for i in range(pieces):
        rows = slice(i * size, (i + 1) * size)
        out.append(sum_heads(near[rows] + flip(far_low[rows], "seq", 2).astype(F32)))
    return jnp.concatenate(out, axis=0) if pieces > 1 else out[0]


def on_device(
    hidden_in,
    segment_ids,
    position_ids,
    out_cot,
    attn_gain,
    w_query,
    b_query,
    w_key,
    b_key,
    w_value,
    b_value,
    w_out,
    ffn_gain,
    w_gate,
    w_up,
    w_down,
):
    row_count, row_width, model_width = hidden_in.shape
    tokens = row_count * row_width
    heads, head_size = b_query.shape
    wide = heads * head_size
    factor = head_size ** (-0.5)
    places = lax.axis_size("seq")
    columns = places // 4
    core = lax.axis_index("dp")
    place = lax.axis_index("seq")
    head = lax.axis_index("head")
    column = place // 4
    level = (place // 2) % 2
    side = place % 2
    shard = w_gate.shape[0]
    units = w_gate.shape[1]
    block = -(-units // (4 * LANES)) * LANES

    gain_one = attn_gain.astype(F32)
    marks_own = jnp.concatenate([segment_ids, position_ids], axis=0)
    full_qkv, full_out, marks_all, near_gate, near_up, near_down, normed = gather_pieces(
        [jnp.concatenate([w_query, w_key, w_value], axis=1), w_out.T, marks_own],
        (1, 1, 0),
        0,
        (w_gate, w_up, w_down.T),
        block,
        (hidden_in, gain_one[None]),
    )
    normed = normed.reshape(tokens, model_width)
    full_qkv = full_qkv.reshape(model_width, -1)
    full_out = full_out.reshape(model_width, -1)
    marks_all = marks_all.reshape(places, 2, row_count, row_width).transpose(1, 2, 0, 3)
    marks_all = marks_all.reshape(2, row_count, 1, places * row_width)
    marks = (
        segment_ids[:, :, None],
        position_ids[:, :, None],
        marks_all[0],
        marks_all[1],
    )

    def column_gather(own):
        return [own] + [flip(own, "seq", 4 * k) for k in range(1, columns)]

    def side_gather(parts):
        pieces = []
        for part in parts:
            pieces += [part, flip(part, "seq", 1)]
        return join_pieces(pieces)

    gate_parts = column_gather(near_gate)

    hidden = hidden_in.reshape(tokens, model_width).astype(F32)
    scale_one = norm_scale(hidden)
    cosine, sine_table = rope_tables(position_ids.reshape(tokens), head_size)
    bias = jnp.concatenate([b_query.reshape(-1), b_key.reshape(-1), b_value.reshape(-1)])
    qkv = plain_dot(normed, full_qkv) + bias.astype(F32)
    queries = rotate(
        qkv[:, :wide].reshape(tokens, heads, head_size),
        cosine[:, None, :],
        sine_table[:, None, :],
        1.0,
    ).astype(BF16)
    queries = queries.reshape(row_count, row_width, wide)
    key_rot = rotate(qkv[:, wide : wide + head_size], cosine, sine_table, 1.0).astype(BF16)
    local_kv = jnp.concatenate([key_rot, qkv[:, wide + head_size :].astype(BF16)], axis=-1)
    local_kv = local_kv.reshape(row_count, row_width, 2 * head_size)
    (all_kv,) = gather_pieces([local_kv], (0,), 1)

    up_parts = column_gather(after(near_up, all_kv))
    full_gate = side_gather(gate_parts)
    full_up = side_gather(up_parts)

    out_other = flip(full_out, "head", 1)
    out_all = in_order(full_out, out_other, head, 1)

    mixed = attend(queries, all_kv, marks, heads, head_size, factor).reshape(tokens, wide)
    mixed_all = in_order(mixed, flip(mixed, "head", 1), head, 1)
    middle = hidden + through_weight(mixed_all, out_all)
    scale_two = norm_scale(middle)
    gain_two = ffn_gain.astype(F32)
    normed_own = (middle * scale_two * gain_two).astype(BF16)
    normed_far = far_rows(normed_own, head)

    down_parts = column_gather(after(near_down, normed_own))
    full_down = side_gather(down_parts)

    live_rows = (segment_ids != 0).astype(F32).reshape(tokens, 1)
    cotangent = out_cot.reshape(tokens, model_width).astype(F32) * live_rows
    cot_own = cotangent.astype(BF16)
    cot_far = far_rows(after(cot_own, normed_own), head)

    drawn_back = 4 * block - units
    live_units = (jnp.arange(block) >= drawn_back) | (level * 2 + core < 3)
    forward, backward, norms, cots = [], [], [], []
    for own_rows, own_cot in ((normed_own, cot_own), (normed_far, cot_far)):
        rows = both_cores(own_rows)
        gate_pre = jnp.where(live_units, plain_dot(rows, full_gate), 0.0)
        up_pre = jnp.where(live_units, plain_dot(rows, full_up), 0.0)
        sigmoid_gate = jax.nn.sigmoid(gate_pre)
        activated = gate_pre * sigmoid_gate
        product = (activated * up_pre).astype(BF16)
        cot_rows = both_cores(own_cot)
        d_product = plain_dot(cot_rows, full_down).astype(BF16).astype(F32)
        slope = sigmoid_gate * (1.0 + gate_pre * (1.0 - sigmoid_gate))
        d_gate = (d_product * up_pre * slope).astype(BF16)
        d_up = (d_product * activated).astype(BF16)
        norms.append(rows)
        cots.append(cot_rows)
        forward.append(product)
        backward.append((d_gate, d_up))
    back_parts = [
        through_weight(d_gate, full_gate) + through_weight(d_up, full_up)
        for d_gate, d_up in backward
    ]
    back_two = collect(*back_parts, 2)

    def weight_grad(lefts, rights):
        return (
            grad_of_weight(lefts[0], rights[0]) + grad_of_weight(lefts[1], rights[1])
        ).astype(BF16)

    grad_down = weight_grad(cots, forward)
    grad_gate = weight_grad(norms, [pair[0] for pair in backward])
    grad_up = weight_grad(norms, [pair[1] for pair in backward])
    result = middle + collect(*[through_weight(part, full_down) for part in forward], 1)
    layer_out = result.astype(BF16).reshape(row_count, row_width, model_width)

    ffn_sums = []
    for grad in (grad_down, grad_gate, grad_up):
        blocks = grad.reshape(2, columns, 2, 2, shard, block)
        half = take(blocks, side, 3).astype(F32)
        half = half + flip(take(blocks, 1 - side, 3), "seq", 1).astype(F32)
        low = half.astype(BF16)
        total = take(half, column, 1)
        for k in range(1, columns):
            total = total + flip(take(low, column ^ k, 1), "seq", 4 * k).astype(F32)
        ffn_sums.append(total.astype(BF16))

    gain_two_grad = jnp.sum(back_two * middle * scale_two, axis=0)
    d_middle = cotangent + norm_back(back_two, middle, scale_two, gain_two)
    d_middle_low = d_middle.astype(BF16)
    d_mixed = plain_dot(d_middle_low, full_out).astype(BF16)

    turns = (
        jnp.concatenate([cosine, cosine], axis=1).reshape(row_count, row_width, head_size),
        jnp.concatenate([sine_table, -sine_table], axis=1).reshape(
            row_count, row_width, head_size
        ),
    )
    d_query, d_kv_all = attend_back(
        queries,
        d_mixed.reshape(row_count, row_width, wide),
        all_kv,
        marks,
        turns,
        heads,
        head_size,
        factor,
    )
    (d_kv,) = reduce_pieces([d_kv_all], (0,), None, 2)
    d_kv = d_kv.reshape(tokens, 2 * head_size)
    d_key = rotate(d_kv[:, :head_size], cosine, sine_table, -1.0).astype(BF16)
    d_value = d_kv[:, head_size:].astype(BF16)
    d_qkv = jnp.concatenate([d_query.reshape(tokens, wide), d_key, d_value], axis=-1)
    back_part = through_weight(d_qkv, full_qkv)
    gain_one_part = jnp.sum(back_part * hidden * scale_one, axis=0)
    back_low = lax.reduce_precision(back_part, 8, 7).astype(BF16)
    back_other = after(flip(back_low, "head", 1), gain_one_part)
    back_one = back_low.astype(F32) + back_other.astype(F32)
    d_hidden = d_middle + norm_back(back_one, hidden, scale_one, gain_one)
    input_grad = d_hidden.astype(BF16).reshape(row_count, row_width, model_width)

    bias_grad = jnp.sum(d_qkv.astype(F32), axis=0)
    vectors = jnp.concatenate([bias_grad, gain_two_grad, gain_one_part])
    first_row = (vectors.size - model_width) // LANES
    qkv_grad = grad_of_weight(normed, d_qkv).astype(BF16).reshape(2 * places, shard, -1)
    out_grad = grad_of_weight(d_middle_low, mixed).astype(BF16).reshape(2 * places, shard, -1)
    qkv_sum, out_sum, vectors, down_sum, gate_sum, up_sum = reduce_pieces(
        [qkv_grad, out_grad], (1, 1), vectors.reshape(-1, LANES), 3, first_row, ffn_sums, units
    )
    out_sum = out_sum.T
    down_sum = down_sum.T
    vectors = vectors.reshape(-1)
    index = core * places + place
    replicas = 2 * places
    narrow = head_size // replicas
    bias_sums = vectors[: wide + 2 * head_size].reshape(heads + 2, head_size)
    bias_mine = lax.dynamic_slice_in_dim(bias_sums, index * narrow, narrow, 1)
    gains = vectors[wide + 2 * head_size :].reshape(2, replicas, model_width // replicas)
    gains_mine = take(gains, index, 1)
    return (
        layer_out,
        input_grad,
        gains_mine[1],
        qkv_sum[:, :wide],
        bias_mine[:heads],
        qkv_sum[:, wide : wide + head_size],
        bias_sums[heads : heads + 1],
        qkv_sum[:, wide + head_size :],
        bias_mine[heads + 1 :],
        out_sum,
        gains_mine[0],
        gate_sum,
        up_sum,
        down_sum,
    )


def solution(mesh):
    placed = (
        P("dp", "seq", None),
        P("dp", "seq"),
        P("dp", "seq"),
        P("dp", "seq", None),
        P(),
        P(("dp", "seq"), "head"),
        P("head", None),
        P(("dp", "seq"), "head"),
        P("head", None),
        P(("dp", "seq"), "head"),
        P("head", None),
        P("head", ("dp", "seq")),
        P(),
        P(("dp", "seq"), "head"),
        P(("dp", "seq"), "head"),
        P("head", ("dp", "seq")),
    )
    return jax.shard_map(
        on_device,
        mesh=mesh,
        in_specs=placed,
        out_specs=(
            P("dp", "seq", None),
            P("dp", "seq", None),
            P(("dp", "seq")),
            P(("dp", "seq"), "head"),
            P("head", ("dp", "seq")),
            P(("dp", "seq"), "head"),
            P("head", None),
            P(("dp", "seq"), "head"),
            P("head", ("dp", "seq")),
            P("head", ("dp", "seq")),
            P(("dp", "seq")),
            P(("dp", "seq"), "head"),
            P(("dp", "seq"), "head"),
            P("head", ("dp", "seq")),
        ),
        check_vma=False,
    )
```

```python
import functools

import jax
import jax.numpy as jnp
from jax import lax
from jax.experimental import pallas as pl
from jax.experimental.pallas import tpu as pltpu
from jax.sharding import PartitionSpec as P


EPSILON = 1e-06
THETA = 1000000.0
MASKED = -1e30
LANES = 128
BF16 = jnp.bfloat16
F32 = jnp.float32
MESH = pl.DeviceIdType.MESH


def rope_tables(position, head_size):
    half_size = head_size // 2
    frequency = THETA ** (-jnp.arange(half_size, dtype=F32) * 2.0 / head_size)
    angles = position.astype(F32)[:, None] * frequency[None, :]
    return jnp.cos(angles), jnp.sin(angles)


def rotate(values, cosine, sine_table, direction):
    half_size = values.shape[-1] // 2
    first_half = values[..., :half_size]
    second_half = values[..., half_size:]
    return jnp.concatenate(
        [
            first_half * cosine - direction * (second_half * sine_table),
            second_half * cosine + direction * (first_half * sine_table),
        ],
        axis=-1,
    )


def xor(index, mask):
    out = index
    bit = 1
    while bit <= mask:
        if mask & bit:
            out = out + bit - 2 * bit * lax.rem(lax.div(index, bit), 2)
        bit *= 2
    return out


def plain_dot(left, right):
    return jnp.dot(left, right, preferred_element_type=F32)


def grad_of_weight(left, right):
    return lax.dot_general(left, right, (((0,), (0,)), ((), ())), preferred_element_type=F32)


def through_weight(left, right):
    return lax.dot_general(left, right, (((1,), (1,)), ((), ())), preferred_element_type=F32)


def norm_scale(values):
    return lax.rsqrt(jnp.mean(values * values, axis=-1, keepdims=True) + EPSILON)


def norm_back(grad_in, values, scale_rows, gain):
    scaled = grad_in * gain
    cubed = scale_rows * scale_rows * scale_rows
    return scale_rows * scaled - values * cubed * jnp.mean(scaled * values, axis=-1, keepdims=True)


def flip(values, axis, mask):
    size = lax.axis_size(axis)
    return lax.ppermute(values, axis, [(i, i ^ mask) for i in range(size)])


def after(values, gate):
    return lax.optimization_barrier((values, gate))[0]


def take(buffer, index, axis=0):
    return lax.dynamic_index_in_dim(buffer, index, axis, keepdims=False)


def allowed_keys(seg_q, pos_q, seg_k, pos_k):
    return (seg_q == seg_k) & (pos_k <= pos_q)


def dot_nt(left, right):
    return lax.dot_general(left, right, (((1,), (1,)), ((), ())), preferred_element_type=F32)


def dot_tn(left, right):
    return lax.dot_general(left, right, (((0,), (0,)), ((), ())), preferred_element_type=F32)


def probabilities(query, keys, allowed, factor):
    scores = jnp.where(allowed, dot_nt(query, keys) * factor, MASKED)
    top = jnp.max(scores, axis=-1, keepdims=True)
    terms = jnp.where(allowed, jnp.exp(scores - top), 0.0)
    return terms / jnp.sum(terms, axis=-1, keepdims=True)


def attend_kernel(heads, head_size, factor, q_ref, kv_ref, sq_ref, pq_ref, sk_ref, pk_ref, o_ref):
    allowed = allowed_keys(sq_ref[0], pq_ref[0], sk_ref[0], pk_ref[0])
    joint = kv_ref[:, 0].reshape(-1, 2 * head_size)
    keys = joint[:, :head_size]
    values = joint[:, head_size:]
    for head in range(heads):
        lanes = slice(head * head_size, (head + 1) * head_size)
        probs = probabilities(q_ref[0, :, lanes], keys, allowed, factor)
        o_ref[0, :, lanes] = jnp.dot(
            probs.astype(BF16), values, preferred_element_type=F32
        ).astype(BF16)


def attend_back_kernel(
    heads, head_size, factor, q_ref, do_ref, kv_ref, sq_ref, pq_ref, sk_ref, pk_ref,
    cos_ref, sin_ref, dq_ref, dkv_ref, acc
):
    allowed = allowed_keys(sq_ref[0], pq_ref[0], sk_ref[0], pk_ref[0])
    joint = kv_ref[:, 0].reshape(-1, 2 * head_size)
    keys = joint[:, :head_size]
    values = joint[:, head_size:]
    for head in range(heads):
        lanes = slice(head * head_size, (head + 1) * head_size)
        query = q_ref[0, :, lanes]
        d_out = do_ref[0, :, lanes]
        probs = probabilities(query, keys, allowed, factor)
        d_probs = dot_nt(d_out, values)
        delta = jnp.sum(probs * d_probs, axis=-1, keepdims=True)
        d_scores = (probs * (d_probs - delta)).astype(BF16)
        d_query = jnp.dot(d_scores, keys, preferred_element_type=F32) * factor
        turned = pltpu.roll(d_query, head_size // 2, 1)
        dq_ref[0, :, lanes] = (d_query * cos_ref[0] + turned * sin_ref[0]).astype(BF16)
        d_key = dot_tn(d_scores, query) * factor
        d_value = dot_tn(probs.astype(BF16), d_out)
        if head == 0:
            acc[:, :head_size] = d_key
            acc[:, head_size:] = d_value
        else:
            acc[:, :head_size] += d_key
            acc[:, head_size:] += d_value
    dkv_ref[:, 0] = acc[...].astype(BF16).reshape(dkv_ref.shape[0], -1, 2 * head_size)


def row_spec(*shape):
    return pl.BlockSpec((1,) + shape, lambda row: (row,) + (0,) * len(shape))


def keys_spec(places, *shape):
    return pl.BlockSpec(
        (places, 1) + shape, lambda row: (0, row) + (0,) * len(shape)
    )


def attend(queries, all_kv, marks, heads, head_size, factor):
    rows, width, wide = queries.shape
    places = all_kv.shape[0]
    length = places * width
    return pl.pallas_call(
        functools.partial(attend_kernel, heads, head_size, factor),
        grid=(rows,),
        out_shape=jax.ShapeDtypeStruct((rows, width, wide), BF16),
        in_specs=[
            row_spec(width, wide),
            keys_spec(places, width, 2 * head_size),
            row_spec(width, 1),
            row_spec(width, 1),
            row_spec(1, length),
            row_spec(1, length),
        ],
        out_specs=row_spec(width, wide),
        cost_estimate=pl.CostEstimate(
            flops=4 * rows * width * wide * length,
            bytes_accessed=4 * rows * (width * wide + length * head_size),
            transcendentals=rows * width * heads * length,
        ),
        name="attend",
    )(queries, all_kv, *marks)


def attend_back(queries, d_mixed, all_kv, marks, turns, heads, head_size, factor):
    rows, width, wide = queries.shape
    places = all_kv.shape[0]
    length = places * width
    return pl.pallas_call(
        functools.partial(attend_back_kernel, heads, head_size, factor),
        grid=(rows,),
        out_shape=(
            jax.ShapeDtypeStruct((rows, width, wide), BF16),
            jax.ShapeDtypeStruct((places, rows, width, 2 * head_size), BF16),
        ),
        in_specs=[
            row_spec(width, wide),
            row_spec(width, wide),
            keys_spec(places, width, 2 * head_size),
            row_spec(width, 1),
            row_spec(width, 1),
            row_spec(1, length),
            row_spec(1, length),
            row_spec(width, head_size),
            row_spec(width, head_size),
        ],
        out_specs=(row_spec(width, wide), keys_spec(places, width, 2 * head_size)),
        scratch_shapes=[pltpu.VMEM((length, 2 * head_size), F32)],
        cost_estimate=pl.CostEstimate(
            flops=10 * rows * width * wide * length,
            bytes_accessed=8 * rows * (width * wide + length * head_size),
            transcendentals=rows * width * heads * length,
        ),
        name="attend_back",
    )(queries, d_mixed, all_kv, *marks, *turns)


def partners_of(core, place, head, planes, over_core):
    found = [(core, xor(place, 2 * k), head) for k in range(1, planes)]
    found.append((core, xor(place, 1), head))
    if over_core:
        found.append((1 - core, place, head))
    return found


def greet(partners):
    barrier = pltpu.get_barrier_semaphore()
    for device in partners:
        pl.semaphore_signal(barrier, inc=1, device_id=device, device_id_type=MESH)
    pl.semaphore_wait(barrier, len(partners))


def remote(source, target, send_sem, recv_sem, device):
    copy = pltpu.make_async_remote_copy(
        src_ref=source,
        dst_ref=target,
        send_sem=send_sem,
        recv_sem=recv_sem,
        device_id=device,
        device_id_type=MESH,
    )
    copy.start()
    return copy


def quarter_start(which, block, units):
    return pl.multiple_of(which * block - lax.div(which, 3) * (4 * block - units), LANES)


def gather_kernel(places, flags, extra, block, normed, *refs):
    count = len(flags)
    sources, refs = refs[:count], refs[count:]
    weights, refs = refs[:extra], refs[extra:]
    if normed:
        (hidden_ref, gain_ref), refs = refs[:2], refs[2:]
    outs, refs = refs[:count], refs[count:]
    nears, refs = refs[:extra], refs[extra:]
    if normed:
        normed_ref, refs = refs[0], refs[1:]
    own_sem, send_z, recv_z, send_y, recv_y, send_c, recv_c, send_q, recv_q = refs
    core, place, head = lax.axis_index("dp"), lax.axis_index("seq"), lax.axis_index("head")
    planes = places // 2

    def slot(n, mask):
        where = xor(place, mask)
        return outs[n].at[core * places + where if flags[n] else where]

    partners = partners_of(core, place, head, planes, any(flags))
    if extra:
        partners.append((1 - core, xor(place, 2), head))
    greet(partners)
    near = (core, xor(place, 1), head)
    other = (1 - core, place, head)
    along, across, over, quarter = {}, {}, {}, {}
    for n in range(count):
        for k in range(1, planes):
            along[n, k] = remote(
                sources[n],
                slot(n, 0),
                send_z.at[n, k],
                recv_z.at[n, k],
                (core, xor(place, 2 * k), head),
            )
    local = []
    for n in range(count):
        across[n, 0] = remote(
            sources[n], slot(n, 0), send_y.at[n, 0], recv_y.at[n, 0], near
        )
        if flags[n]:
            over[n, 0] = remote(
                sources[n], slot(n, 0), send_c.at[n, 0], recv_c.at[n, 0], other
            )
        copy = pltpu.make_async_copy(sources[n], slot(n, 0), own_sem.at[n])
        copy.start()
        local.append(copy)
    for n in range(extra):
        units = weights[n].shape[1]
        for m in range(4):
            to_core = core if m % 2 == 0 else 1 - core
            to_place = xor(place, m // 2 * 2)
            which = lax.rem(lax.div(to_place, 2), 2) * 2 + to_core
            piece = weights[n].at[:, pl.ds(quarter_start(which, block, units), block)]
            if m:
                quarter[n, m] = remote(
                    piece,
                    nears[n].at[m],
                    send_q.at[n, m],
                    recv_q.at[n, m],
                    (to_core, to_place, head),
                )
            else:
                copy = pltpu.make_async_copy(piece, nears[n].at[0], send_q.at[n, 0])
                copy.start()
                local.append(copy)
    if normed:
        for row in range(hidden_ref.shape[0]):
            values = hidden_ref[row].astype(F32)
            normed_ref[row] = (values * norm_scale(values) * gain_ref[...]).astype(BF16)
    for n in range(count):
        for k in range(1, planes):
            along[n, k].wait_recv()
            piece = slot(n, 2 * k)
            across[n, k] = remote(piece, piece, send_y.at[n, k], recv_y.at[n, k], near)
            if flags[n]:
                over[n, 2 * k] = remote(
                    piece, piece, send_c.at[n, 2 * k], recv_c.at[n, 2 * k], other
                )
    for n in range(count):
        for k in range(planes):
            across[n, k].wait_recv()
            if flags[n]:
                mask = 2 * k + 1
                piece = slot(n, mask)
                over[n, mask] = remote(
                    piece, piece, send_c.at[n, mask], recv_c.at[n, mask], other
                )
    for copies in (over, quarter):
        for copy in copies.values():
            copy.wait_recv()
    for copies in (along, across, over, quarter):
        for copy in copies.values():
            copy.wait_send()
    for copy in local:
        copy.wait()


def gather_pieces(pieces, flags, ident, weights=(), block=0, norm=None):
    places = lax.axis_size("seq")
    planes = places // 2
    count, extra = len(pieces), len(weights)
    out_shape = [
        jax.ShapeDtypeStruct(((1 + flag) * places,) + piece.shape, piece.dtype)
        for piece, flag in zip(pieces, flags)
    ]
    out_shape += [jax.ShapeDtypeStruct((4, w.shape[0], block), w.dtype) for w in weights]
    out_specs = [pl.BlockSpec(memory_space=pl.ANY)] * (count + extra)
    operands = list(pieces) + list(weights)
    if norm is not None:
        operands += list(norm)
        out_shape.append(jax.ShapeDtypeStruct(norm[0].shape, BF16))
        out_specs.append(pl.BlockSpec(memory_space=pltpu.VMEM))
    quarters = (max(extra, 1), 4)
    return pl.pallas_call(
        functools.partial(gather_kernel, places, flags, extra, block, norm is not None),
        out_shape=tuple(out_shape),
        in_specs=[pl.BlockSpec(memory_space=pltpu.VMEM)] * len(operands),
        out_specs=tuple(out_specs),
        scratch_shapes=[
            pltpu.SemaphoreType.DMA((count,)),
            pltpu.SemaphoreType.DMA((count, planes)),
            pltpu.SemaphoreType.DMA((count, planes)),
            pltpu.SemaphoreType.DMA((count, planes)),
            pltpu.SemaphoreType.DMA((count, planes)),
            pltpu.SemaphoreType.DMA((count, places)),
            pltpu.SemaphoreType.DMA((count, places)),
            pltpu.SemaphoreType.DMA(quarters),
            pltpu.SemaphoreType.DMA(quarters),
        ],
        compiler_params=pltpu.CompilerParams(collective_id=ident, has_side_effects=True),
        cost_estimate=pl.CostEstimate(flops=0, bytes_accessed=100_000_000, transcendentals=0),
    )(*operands)


def reduce_kernel(places, flags, vector, first_row, extra, block, *refs):
    count = len(flags)
    planes = places // 2
    step = count + vector
    grads, refs = refs[:step], refs[step:]
    pieces, refs = refs[:extra], refs[extra:]
    totals, refs = refs[:step], refs[step:]
    wholes, refs = refs[:extra], refs[extra:]
    sems, refs = refs[:8], refs[8:]
    send_c, recv_c, send_y, recv_y, send_z, recv_z, send_q, recv_q = sems
    got_c, got_y, got_z, out_y, out_z = (refs[i * step : (i + 1) * step] for i in range(5))
    refs = refs[5 * step :]
    got_q, refs = refs[:extra], refs[extra:]
    core, place, head = lax.axis_index("dp"), lax.axis_index("seq"), lax.axis_index("head")
    level = lax.rem(lax.div(place, 2), 2)
    partners = partners_of(core, place, head, planes, any(flags))
    if extra:
        partners.append((1 - core, xor(place, 2), head))
    if vector:
        partners.append((core, place, 1 - head))
    greet(partners)
    near = (core, xor(place, 1), head)
    other = (1 - core, place, head)
    over, across, along, quarter = {}, {}, {}, {}
    order = [2 * k + 1 for k in range(planes)] + [2 * k for k in range(1, planes)] + [0]

    if vector:
        got_x, sum_x, sem_x = refs
        facing = remote(
            grads[count], got_x, sem_x.at[0], sem_x.at[1], (core, place, 1 - head)
        )
    for n in range(count):
        if flags[n]:
            for mask in order:
                over[n, mask] = remote(
                    grads[n].at[(1 - core) * places + xor(place, mask)],
                    got_c[n].at[mask],
                    send_c.at[n, mask],
                    recv_c.at[n, mask],
                    other,
                )
    for n in range(extra):
        for m in range(1, 4):
            to_core = core if m % 2 == 0 else 1 - core
            to_place = xor(place, m // 2 * 2)
            quarter[n, m] = remote(
                pieces[n].at[to_core, lax.rem(lax.div(to_place, 2), 2)],
                got_q[n].at[m],
                send_q.at[n, m],
                recv_q.at[n, m],
                (to_core, to_place, head),
            )

    def chip_sum(n, mask):
        where = xor(place, mask)
        if not flags[n]:
            return grads[n][where].astype(F32)
        over[n, mask].wait_recv()
        return grads[n][core * places + where].astype(F32) + got_c[n][mask].astype(F32)

    if vector:
        facing.wait_recv()
        rows = lax.broadcasted_iota(jnp.int32, got_x.shape, 0)
        sum_x[...] = grads[count][...] + jnp.where(rows >= first_row, got_x[...], 0.0)
        over[count, 0] = remote(
            sum_x, got_c[count], send_c.at[count, 0], recv_c.at[count, 0], other
        )
    for n in range(count):
        for k in list(range(1, planes)) + [0]:
            out_y[n][k] = chip_sum(n, 2 * k + 1).astype(BF16)
            across[n, k] = remote(
                out_y[n].at[k], got_y[n].at[k], send_y.at[n, k], recv_y.at[n, k], near
            )
    if vector:
        over[count, 0].wait_recv()
        out_y[count][...] = sum_x[...] + got_c[count][...]
        across[count, 0] = remote(
            out_y[count], got_y[count], send_y.at[count, 0], recv_y.at[count, 0], near
        )
    for n in range(extra):
        wholes[n][...] = jnp.zeros_like(wholes[n])
        units = wholes[n].shape[1]
        columns = pl.ds(quarter_start(level * 2 + core, block, units), block)
        wholes[n][:, columns] += pieces[n][core, level].astype(F32)
    for n in range(count):
        for k in range(1, planes):
            part = chip_sum(n, 2 * k)
            across[n, k].wait_recv()
            out_z[n][k] = (part + got_y[n][k].astype(F32)).astype(BF16)
            along[n, k] = remote(
                out_z[n].at[k],
                got_z[n].at[k],
                send_z.at[n, k],
                recv_z.at[n, k],
                (core, xor(place, 2 * k), head),
            )
    if vector:
        across[count, 0].wait_recv()
        out_z[count][...] = out_y[count][...] + got_y[count][...]
        for k in range(1, planes):
            along[count, k] = remote(
                out_z[count],
                got_z[count].at[k],
                send_z.at[count, k],
                recv_z.at[count, k],
                (core, xor(place, 2 * k), head),
            )
    for n in range(extra):
        units = wholes[n].shape[1]
        for m in range(1, 4):
            to_core = core if m % 2 == 0 else 1 - core
            which = (level if m < 2 else 1 - level) * 2 + to_core
            quarter[n, m].wait_recv()
            columns = pl.ds(quarter_start(which, block, units), block)
            wholes[n][:, columns] += got_q[n][m].astype(F32)
    for n in range(count):
        part = chip_sum(n, 0)
        across[n, 0].wait_recv()
        totals[n][...] = part + got_y[n][0].astype(F32)
    if vector:
        totals[count][...] = out_z[count][...]
    for n in range(step):
        for k in range(1, planes):
            along[n, k].wait_recv()
            totals[n][...] += got_z[n][k].astype(F32)
    if vector:
        facing.wait_send()
    for copies in (over, across, along, quarter):
        for copy in copies.values():
            copy.wait_send()


def reduce_pieces(grads, flags, vector, ident, first_row=0, pieces=(), units=0):
    places = lax.axis_size("seq")
    planes = places // 2
    count, extra = len(grads), len(pieces)
    shapes = [grad.shape[1:] for grad in grads]
    operands = list(grads)
    step = count
    if vector is not None:
        operands.append(vector)
        step += 1
    operands += list(pieces)
    block = pieces[0].shape[-1] if extra else 0
    small = (8, LANES)

    def buffers(leading, vector_leading):
        out = [pltpu.VMEM(leading + shape, BF16) for shape in shapes]
        if vector is not None:
            out.append(pltpu.VMEM(vector_leading + vector.shape, F32))
        return out

    got_c = [
        pltpu.VMEM(((places,) + shape) if flag else small, BF16)
        for shape, flag in zip(shapes, flags)
    ]
    if vector is not None:
        got_c.append(pltpu.VMEM(vector.shape, F32))
    quarters = (max(extra, 1), 4)
    scratch = (
        [
            pltpu.SemaphoreType.DMA((step, places)),
            pltpu.SemaphoreType.DMA((step, places)),
            pltpu.SemaphoreType.DMA((step, planes)),
            pltpu.SemaphoreType.DMA((step, planes)),
            pltpu.SemaphoreType.DMA((step, planes)),
            pltpu.SemaphoreType.DMA((step, planes)),
            pltpu.SemaphoreType.DMA(quarters),
            pltpu.SemaphoreType.DMA(quarters),
        ]
        + got_c
        + buffers((planes,), ())
        + buffers((planes,), (planes,))
        + buffers((planes,), ())
        + buffers((planes,), ())
        + [pltpu.VMEM((4,) + piece.shape[2:], BF16) for piece in pieces]
    )
    out_shapes = [jax.ShapeDtypeStruct(shape, F32) for shape in shapes]
    if vector is not None:
        scratch += [
            pltpu.VMEM(vector.shape, F32),
            pltpu.VMEM(vector.shape, F32),
            pltpu.SemaphoreType.DMA((2,)),
        ]
        out_shapes.append(jax.ShapeDtypeStruct(vector.shape, F32))
    out_shapes += [jax.ShapeDtypeStruct((piece.shape[2], units), F32) for piece in pieces]
    return pl.pallas_call(
        functools.partial(
            reduce_kernel, places, flags, int(vector is not None), first_row, extra, block
        ),
        out_shape=tuple(out_shapes),
        in_specs=[pl.BlockSpec(memory_space=pltpu.VMEM)] * len(operands),
        out_specs=tuple([pl.BlockSpec(memory_space=pltpu.VMEM)] * len(out_shapes)),
        scratch_shapes=scratch,
        compiler_params=pltpu.CompilerParams(collective_id=ident, has_side_effects=True),
        cost_estimate=pl.CostEstimate(flops=0, bytes_accessed=100_000_000, transcendentals=0),
    )(*operands)


def join_kernel(places, count, *refs):
    pieces, out, held, in_sem, out_sem = refs[:count], *refs[count:]
    core, place = lax.axis_index("dp"), lax.axis_index("seq")
    arriving = []
    for p in range(count):
        for q in range(4):
            i = 4 * p + q
            copy = pltpu.make_async_copy(pieces[p].at[q], held.at[i], in_sem.at[i])
            copy.start()
            arriving.append(copy)
    leaving = []
    for p in range(count):
        for q in range(4):
            i = 4 * p + q
            arriving[i].wait()
            mask = 4 * (p // 2) + 2 * (q // 2) + p % 2
            where = (core if q % 2 == 0 else 1 - core) * places + xor(place, mask)
            copy = pltpu.make_async_copy(held.at[i], out.at[where], out_sem.at[i])
            copy.start()
            leaving.append(copy)
    for copy in leaving:
        copy.wait()


def join_pieces(pieces):
    places = lax.axis_size("seq")
    count = len(pieces)
    _, rows, columns = pieces[0].shape
    total = 4 * count
    out = pl.pallas_call(
        functools.partial(join_kernel, places, count),
        out_shape=jax.ShapeDtypeStruct((total, rows, columns), BF16),
        in_specs=[pl.BlockSpec(memory_space=pl.ANY)] * count,
        out_specs=pl.BlockSpec(memory_space=pl.ANY),
        scratch_shapes=[
            pltpu.VMEM((total, rows, columns), BF16),
            pltpu.SemaphoreType.DMA((total,)),
            pltpu.SemaphoreType.DMA((total,)),
        ],
        cost_estimate=pl.CostEstimate(
            flops=0, bytes_accessed=4 * total * rows * columns, transcendentals=0
        ),
        name="join",
    )(*pieces)
    return out.reshape(total * rows, columns)


def unit_chunk(block):
    third = block // 3
    return third if block % 3 == 0 and third % LANES == 0 else LANES


def ffn_forward_kernel(rows_ref, live_ref, gate_ref, up_ref, g_ref, u_ref, z_ref):
    block = gate_ref.shape[1]
    chunk = unit_chunk(block)

    def step(j, carry):
        part = pl.ds(pl.multiple_of(j * chunk, LANES), chunk)
        live = live_ref[:, part] > 0.0
        gate_pre = jnp.where(live, plain_dot(rows_ref[...], gate_ref[:, part]), 0.0)
        up_pre = jnp.where(live, plain_dot(rows_ref[...], up_ref[:, part]), 0.0)
        g_ref[:, part] = gate_pre
        u_ref[:, part] = up_pre
        z_ref[:, part] = (gate_pre * jax.nn.sigmoid(gate_pre) * up_pre).astype(BF16)
        return carry

    lax.fori_loop(0, block // chunk, step, 0)


def ffn_back_kernel(cot_ref, g_ref, u_ref, gate_ref, up_ref, down_ref, dg_ref, du_ref, e_ref):
    width, block = gate_ref.shape
    chunk = unit_chunk(block)

    def step(j, carry):
        part = pl.ds(pl.multiple_of(j * chunk, LANES), chunk)
        d_product = plain_dot(cot_ref[...], down_ref[:, part]).astype(BF16).astype(F32)
        gate_pre = g_ref[:, part]
        sigmoid_gate = jax.nn.sigmoid(gate_pre)
        slope = sigmoid_gate * (1.0 + gate_pre * (1.0 - sigmoid_gate))
        dg_ref[:, part] = (d_product * u_ref[:, part] * slope).astype(BF16)
        du_ref[:, part] = (d_product * (gate_pre * sigmoid_gate)).astype(BF16)
        return carry

    lax.fori_loop(0, block // chunk, step, 0)
    wide_chunk = unit_chunk(width)

    def fold(j, carry):
        part = pl.ds(pl.multiple_of(j * wide_chunk, LANES), wide_chunk)
        e_ref[:, part] = (
            dot_nt(dg_ref[...], gate_ref[part, :]) + dot_nt(du_ref[...], up_ref[part, :])
        ).astype(BF16)
        return carry

    lax.fori_loop(0, width // wide_chunk, fold, 0)


def tile_spec(tile, width):
    return pl.BlockSpec((tile, width), lambda i: (i, 0))


def whole_spec(array):
    return pl.BlockSpec(array.shape, lambda i: (0, 0), pipeline_mode=pl.Buffered(1))


def ffn_forward(rows, live, gate, up):
    count, width = rows.shape
    block = gate.shape[1]
    tile = count // 4
    return pl.pallas_call(
        ffn_forward_kernel,
        grid=(4,),
        out_shape=(
            jax.ShapeDtypeStruct((count, block), F32),
            jax.ShapeDtypeStruct((count, block), F32),
            jax.ShapeDtypeStruct((count, block), BF16),
        ),
        in_specs=[tile_spec(tile, width), whole_spec(live), whole_spec(gate), whole_spec(up)],
        out_specs=(tile_spec(tile, block),) * 3,
        cost_estimate=pl.CostEstimate(
            flops=4 * count * width * block,
            bytes_accessed=10 * count * block + 4 * width * block,
            transcendentals=count * block,
        ),
        name="ffn_forward",
    )(rows, live, gate, up)


def ffn_back(cots, gate_pre, up_pre, gate, up, down):
    count, width = cots.shape
    block = gate.shape[1]
    tile = count // 4
    return pl.pallas_call(
        ffn_back_kernel,
        grid=(4,),
        out_shape=(
            jax.ShapeDtypeStruct((count, block), BF16),
            jax.ShapeDtypeStruct((count, block), BF16),
            jax.ShapeDtypeStruct((count, width), BF16),
        ),
        in_specs=[
            tile_spec(tile, width),
            tile_spec(tile, block),
            tile_spec(tile, block),
            whole_spec(gate),
            whole_spec(up),
            whole_spec(down),
        ],
        out_specs=(tile_spec(tile, block), tile_spec(tile, block), tile_spec(tile, width)),
        cost_estimate=pl.CostEstimate(
            flops=6 * count * width * block,
            bytes_accessed=12 * count * block + 6 * width * block,
            transcendentals=count * block,
        ),
        name="ffn_back",
    )(cots, gate_pre, up_pre, gate, up, down)


def in_order(own, other, head, axis):
    first = head == 0
    return jnp.concatenate(
        [jnp.where(first, own, other), jnp.where(first, other, own)], axis=axis
    )


def far_rows(values, head):
    half = values.shape[0] // 2
    got = flip(lax.dynamic_slice_in_dim(values, head * half, half, 0), "seq", 2)
    other = flip(got, "head", 1)
    return in_order(got, other, head, 0)


def four_rows(own, far):
    blocks = [own, flip(own, "dp", 1), far, flip(far, "dp", 1)]
    return lax.optimization_barrier(jnp.concatenate(blocks, axis=0))


def core_sums(part):
    blocks = part.reshape(4, -1, part.shape[-1])
    far = flip(blocks[3].astype(BF16), "dp", 1)
    near = flip(blocks[1].astype(BF16), "dp", 1)
    return (
        blocks[0].astype(F32) + near.astype(F32),
        blocks[2].astype(F32) + far.astype(F32),
    )


def on_device(
    hidden_in,
    segment_ids,
    position_ids,
    out_cot,
    attn_gain,
    w_query,
    b_query,
    w_key,
    b_key,
    w_value,
    b_value,
    w_out,
    ffn_gain,
    w_gate,
    w_up,
    w_down,
):
    row_count, row_width, model_width = hidden_in.shape
    tokens = row_count * row_width
    heads, head_size = b_query.shape
    wide = heads * head_size
    factor = head_size ** (-0.5)
    places = lax.axis_size("seq")
    columns = places // 4
    core = lax.axis_index("dp")
    place = lax.axis_index("seq")
    head = lax.axis_index("head")
    column = place // 4
    level = (place // 2) % 2
    side = place % 2
    shard = w_gate.shape[0]
    units = w_gate.shape[1]
    block = -(-units // (4 * LANES)) * LANES

    gain_one = attn_gain.astype(F32)
    marks_own = jnp.concatenate([segment_ids, position_ids], axis=0)
    full_qkv, full_out, marks_all, near_gate, near_up, near_down, normed = gather_pieces(
        [jnp.concatenate([w_query, w_key, w_value], axis=1), w_out.T, marks_own],
        (1, 1, 0),
        0,
        (w_gate, w_up, w_down.T),
        block,
        (hidden_in, gain_one[None]),
    )
    normed = normed.reshape(tokens, model_width)
    full_qkv = full_qkv.reshape(model_width, -1)
    full_out = full_out.reshape(model_width, -1)
    marks_all = marks_all.reshape(places, 2, row_count, row_width).transpose(1, 2, 0, 3)
    marks_all = marks_all.reshape(2, row_count, 1, places * row_width)
    marks = (
        segment_ids[:, :, None],
        position_ids[:, :, None],
        marks_all[0],
        marks_all[1],
    )

    def column_gather(own):
        return [own] + [flip(own, "seq", 4 * k) for k in range(1, columns)]

    def side_gather(parts):
        pieces = []
        for part in parts:
            pieces += [part, flip(part, "seq", 1)]
        return join_pieces(pieces)

    gate_parts = column_gather(near_gate)

    hidden = hidden_in.reshape(tokens, model_width).astype(F32)
    scale_one = norm_scale(hidden)
    cosine, sine_table = rope_tables(position_ids.reshape(tokens), head_size)
    bias = jnp.concatenate([b_query.reshape(-1), b_key.reshape(-1), b_value.reshape(-1)])
    qkv = plain_dot(normed, full_qkv) + bias.astype(F32)
    queries = rotate(
        qkv[:, :wide].reshape(tokens, heads, head_size),
        cosine[:, None, :],
        sine_table[:, None, :],
        1.0,
    ).astype(BF16)
    queries = queries.reshape(row_count, row_width, wide)
    key_rot = rotate(qkv[:, wide : wide + head_size], cosine, sine_table, 1.0).astype(BF16)
    local_kv = jnp.concatenate([key_rot, qkv[:, wide + head_size :].astype(BF16)], axis=-1)
    local_kv = local_kv.reshape(row_count, row_width, 2 * head_size)
    (all_kv,) = gather_pieces([local_kv], (0,), 1)

    up_parts = column_gather(near_up)
    full_gate = side_gather(gate_parts)
    full_up = side_gather(up_parts)

    out_other = flip(full_out, "head", 1)
    out_all = in_order(full_out, out_other, head, 1)

    live_rows = (segment_ids != 0).astype(F32).reshape(tokens, 1)
    cotangent = out_cot.reshape(tokens, model_width).astype(F32) * live_rows
    cot_own = cotangent.astype(BF16)
    cot_far = far_rows(cot_own, head)

    mixed = attend(queries, all_kv, marks, heads, head_size, factor).reshape(tokens, wide)
    mixed_all = in_order(mixed, flip(mixed, "head", 1), head, 1)
    middle = hidden + through_weight(mixed_all, out_all)
    scale_two = norm_scale(middle)
    gain_two = ffn_gain.astype(F32)
    normed_own = (middle * scale_two * gain_two).astype(BF16)
    normed_far = far_rows(normed_own, head)

    down_parts = column_gather(near_down)
    full_down = side_gather(down_parts)

    drawn_back = 4 * block - units
    live_units = (jnp.arange(block) >= drawn_back) | (level * 2 + core < 3)
    norms = four_rows(normed_own, normed_far)
    cots = four_rows(cot_own, cot_far)
    gate_pre, up_pre, product = ffn_forward(
        norms, live_units.astype(F32)[None], full_gate, full_up
    )
    grad_down = grad_of_weight(cots, product).astype(BF16)
    d_gate, d_up, back_all = ffn_back(
        cots, gate_pre, up_pre, full_gate, full_up, full_down
    )

    near, far = core_sums(back_all)
    far_low = far.astype(BF16)
    halves, crossed = [], []
    for i in range(2):
        rows = slice(i * tokens // 2, (i + 1) * tokens // 2)
        crossed.append(flip(far_low[rows], "seq", 2))
        part = near[rows] + crossed[i].astype(F32)
        low = lax.reduce_precision(part, 8, 7).astype(BF16)
        other = flip(low, "head", 1)
        halves.append(low.astype(F32) + other.astype(F32))
    back_two = jnp.concatenate(halves, axis=0)

    grad_gate = grad_of_weight(norms, d_gate).astype(BF16)
    grad_up = grad_of_weight(norms, d_up).astype(BF16)

    ffn_sums = []
    for grad in (grad_down, grad_gate, grad_up):
        blocks = grad.reshape(2, columns, 2, 2, shard, block)
        got = flip(take(blocks, 1 - side, 3), "seq", 1)
        half = take(blocks, side, 3).astype(F32) + got.astype(F32)
        low = half.astype(BF16)
        total = take(half, column, 1)
        for k in range(1, columns):
            total = total + flip(take(low, column ^ k, 1), "seq", 4 * k).astype(F32)
        ffn_sums.append(total.astype(BF16))

    gain_two_grad = jnp.sum(back_two * middle * scale_two, axis=0)
    d_middle = cotangent + norm_back(back_two, middle, scale_two, gain_two)
    d_middle_low = d_middle.astype(BF16)
    d_mixed = plain_dot(d_middle_low, full_out).astype(BF16)

    result_all = through_weight(product, full_down).astype(BF16)
    near, far = core_sums(result_all)
    half = tokens // 2
    mine = [lax.dynamic_slice_in_dim(part, head * half, half, 0) for part in (near, far)]
    theirs = [
        lax.dynamic_slice_in_dim(part, (1 - head) * half, half, 0) for part in (near, far)
    ]
    got = flip(jnp.concatenate(theirs, axis=0).astype(BF16), "head", 1).astype(F32)
    got_far = flip((mine[1] + got[half:]).astype(BF16), "seq", 2).astype(F32)
    total = mine[0] + got[:half] + got_far
    out_half = (lax.dynamic_slice_in_dim(middle, head * half, half, 0) + total).astype(BF16)
    out_other = flip(out_half, "head", 1)
    layer_out = in_order(out_half, out_other, head, 0)
    layer_out = layer_out.reshape(row_count, row_width, model_width)

    turns = (
        jnp.concatenate([cosine, cosine], axis=1).reshape(row_count, row_width, head_size),
        jnp.concatenate([sine_table, -sine_table], axis=1).reshape(
            row_count, row_width, head_size
        ),
    )
    d_query, d_kv_all = attend_back(
        queries,
        d_mixed.reshape(row_count, row_width, wide),
        all_kv,
        marks,
        turns,
        heads,
        head_size,
        factor,
    )
    (d_kv,) = reduce_pieces([d_kv_all], (0,), None, 2)
    d_kv = d_kv.reshape(tokens, 2 * head_size)
    d_key = rotate(d_kv[:, :head_size], cosine, sine_table, -1.0).astype(BF16)
    d_value = d_kv[:, head_size:].astype(BF16)
    d_qkv = jnp.concatenate([d_query.reshape(tokens, wide), d_key, d_value], axis=-1)
    back_part = through_weight(d_qkv, full_qkv)
    gain_one_part = jnp.sum(back_part * hidden * scale_one, axis=0)
    back_low = lax.reduce_precision(back_part, 8, 7).astype(BF16)
    back_other = after(flip(back_low, "head", 1), gain_one_part)
    back_one = back_low.astype(F32) + back_other.astype(F32)
    d_hidden = d_middle + norm_back(back_one, hidden, scale_one, gain_one)
    input_grad = d_hidden.astype(BF16).reshape(row_count, row_width, model_width)

    bias_grad = jnp.sum(d_qkv.astype(F32), axis=0)
    vectors = jnp.concatenate([bias_grad, gain_two_grad, gain_one_part])
    first_row = (vectors.size - model_width) // LANES
    qkv_grad = grad_of_weight(normed, d_qkv).astype(BF16).reshape(2 * places, shard, -1)
    out_grad = grad_of_weight(d_middle_low, mixed).astype(BF16).reshape(2 * places, shard, -1)
    qkv_sum, out_sum, vectors, down_sum, gate_sum, up_sum = reduce_pieces(
        [qkv_grad, out_grad], (1, 1), vectors.reshape(-1, LANES), 3, first_row, ffn_sums, units
    )
    out_sum = out_sum.T
    down_sum = down_sum.T
    vectors = vectors.reshape(-1)
    index = core * places + place
    replicas = 2 * places
    narrow = head_size // replicas
    bias_sums = vectors[: wide + 2 * head_size].reshape(heads + 2, head_size)
    bias_mine = lax.dynamic_slice_in_dim(bias_sums, index * narrow, narrow, 1)
    gains = vectors[wide + 2 * head_size :].reshape(2, replicas, model_width // replicas)
    gains_mine = take(gains, index, 1)
    return (
        layer_out,
        input_grad,
        gains_mine[1],
        qkv_sum[:, :wide],
        bias_mine[:heads],
        qkv_sum[:, wide : wide + head_size],
        bias_sums[heads : heads + 1],
        qkv_sum[:, wide + head_size :],
        bias_mine[heads + 1 :],
        out_sum,
        gains_mine[0],
        gate_sum,
        up_sum,
        down_sum,
    )


def solution(mesh):
    placed = (
        P("dp", "seq", None),
        P("dp", "seq"),
        P("dp", "seq"),
        P("dp", "seq", None),
        P(),
        P(("dp", "seq"), "head"),
        P("head", None),
        P(("dp", "seq"), "head"),
        P("head", None),
        P(("dp", "seq"), "head"),
        P("head", None),
        P("head", ("dp", "seq")),
        P(),
        P(("dp", "seq"), "head"),
        P(("dp", "seq"), "head"),
        P("head", ("dp", "seq")),
    )
    return jax.shard_map(
        on_device,
        mesh=mesh,
        in_specs=placed,
        out_specs=(
            P("dp", "seq", None),
            P("dp", "seq", None),
            P(("dp", "seq")),
            P(("dp", "seq"), "head"),
            P("head", ("dp", "seq")),
            P(("dp", "seq"), "head"),
            P("head", None),
            P(("dp", "seq"), "head"),
            P("head", ("dp", "seq")),
            P("head", ("dp", "seq")),
            P(("dp", "seq")),
            P(("dp", "seq"), "head"),
            P(("dp", "seq"), "head"),
            P("head", ("dp", "seq")),
        ),
        check_vma=False,
    )
```
